128 devices in a mesh: dp: 64 (over y, z_lo, x, core), rep: 2 (over z_hi).
Axes of the slice: x: 4, y: 4, z: 4 (z_hi: 2, z_lo: 2; z = z_hi * 2 + z_lo), core: 2. Of those that a mesh axis runs over, the one named last changes fastest.
Arguments:
- queries: bfloat16 [8192, 2048], P(('dp', 'rep')), may hold values from -24 to 24
- documents: bfloat16 [8192, 2048], P(('dp', 'rep')), may hold values from -24 to 24
- partner: int32 [8192], P(('dp', 'rep')), may hold values from 0 to 8191, each once
Outputs:
- grad_queries: float32 [8192, 2048], P(('dp', 'rep'))
- grad_documents: float32 [8192, 2048], P(('dp', 'rep'))
The draws below stay inside these ranges and needn't reach their ends.
Inputs may be any that keep to these rules, and one draw needn't show every extreme that they name: `partner`: every document index appears exactly once.
All inputs are finite; a program needn't handle non-finite values.
Results may differ from the reference program's by a relative error of at most 0.0031.
Values may be sent and summed in bfloat16 or wider, within the bound.
A program may use at most 256 MiB of HBM per device.

```python
import math
import jax
import jax.numpy as jnp
from jax import lax

D = 2048
WIDTHS = 9
PAIRS = 8192


def joint_draw(key):
    key_list = jax.random.split(jax.random.fold_in(key, 7), 2)
    query_part = jax.random.normal(key_list[0], (PAIRS, D), jnp.float32)
    document_part = jax.random.normal(key_list[1], (PAIRS, D), jnp.float32)
    return (jnp.clip(query_part, -24.0, 24.0), jnp.clip(document_part, -24.0, 24.0))


def draw_queries(key, part):
    return joint_draw(key)[0].astype(jnp.bfloat16)


def draw_documents(key, part):
    return joint_draw(key)[1].astype(jnp.bfloat16)


def setup_inputs(seed: int = 0) -> dict:
    seeds = jax.random.split(jax.random.key(seed), 4)
    queries = draw_queries(jax.random.fold_in(seeds[3], 71), 0)
    documents = draw_documents(jax.random.fold_in(seeds[3], 71), 0)
    partner = jax.random.permutation(seeds[2], PAIRS).astype(jnp.int32)
    return dict(queries=queries, documents=documents, partner=partner)


logit_gain = 3.0


def reference(queries, documents, partner):
    uppers = [D >> (WIDTHS - 1 - nested) for nested in range(WIDTHS)]
    lowers = [0] + uppers[:-1]
    block_rows = math.gcd(PAIRS, 512)
    block_count = PAIRS // block_rows
    doc_ids = jnp.arange(PAIRS, dtype=jnp.int32)

    def visit_block(doc_grad, block_data):
        rows_q, rows_p = block_data
        target = (rows_p[:, None] == doc_ids[None, :]).astype(jnp.float32)
        suffix = jnp.zeros((block_rows, PAIRS), jnp.float32)
        pieces = [None] * WIDTHS
        for nested in reversed(range(WIDTHS)):
            lower_col = lowers[nested]
            upper_col = uppers[nested]
            scale = logit_gain * upper_col ** -0.5
            logits = jnp.dot(rows_q[:, :upper_col], documents[:, :upper_col].T,
                             preferred_element_type=jnp.float32) * scale
            row_peak = jnp.max(logits, axis=1, keepdims=True)
            row_total = row_peak + jnp.log(jnp.sum(jnp.exp(logits - row_peak), axis=1, keepdims=True))
            suffix = suffix + (jnp.exp(logits - row_total) - target) * scale
            band = suffix.astype(jnp.bfloat16)
            pieces[nested] = jnp.dot(band, documents[:, lower_col:upper_col], preferred_element_type=jnp.float32)
            doc_grad = doc_grad.at[:, lower_col:upper_col].add(
                jnp.dot(band.T, rows_q[:, lower_col:upper_col], preferred_element_type=jnp.float32))
        return doc_grad, jnp.concatenate(pieces, axis=1)

    start_grad = jnp.zeros((PAIRS, D), jnp.float32)
    grad_documents, stacked = lax.scan(
        visit_block, start_grad,
        (queries.reshape(block_count, block_rows, D), partner.reshape(block_count, block_rows)))
    grad_queries = stacked.reshape(PAIRS, D)
    return grad_queries, grad_documents
```

```python
import jax
import jax.numpy as jnp
from jax import lax
from jax.sharding import Mesh
from jax.sharding import PartitionSpec as P

WIDTHS = 9
DP = ("dp_0", "dp_1", "dp_2", "dp_3")
DP_REP = ("dp_0", "dp_1", "dp_2", "dp_3", "rep")


logit_gain = 3.0


def contract(first_op, second_op):
    return lax.dot_general(
        first_op, second_op, (((1,), (1,)), ((), ())), preferred_element_type=jnp.float32
    )


def width_list(feature_dim):
    return [feature_dim >> WIDTHS - 1 - nested for nested in range(WIDTHS)]


def scores(first_op, second_op):
    uppers = width_list(first_op.shape[1])
    result = []
    running = jnp.zeros((first_op.shape[0], second_op.shape[0]), jnp.float32)
    lower_col = 0
    for upper_col in uppers:
        running = running + contract(
            first_op[:, lower_col:upper_col], second_op[:, lower_col:upper_col]
        )
        result.append(running * (logit_gain * upper_col ** (-0.5)))
        lower_col = upper_col
    return result


def band_sums(logit_list, total_list, target, uppers):
    bands = [None] * len(uppers)
    running = None
    for nested in reversed(range(len(uppers))):
        scale = logit_gain * uppers[nested] ** (-0.5)
        weight = (jnp.exp(logit_list[nested] - total_list[nested]) - target) * scale
        running = weight if running is None else running + weight
        bands[nested] = running.astype(jnp.bfloat16)
    return bands


def spread(bands, operand, uppers, transposed):
    pieces = []
    lower_col = 0
    for nested, upper_col in enumerate(uppers):
        block_part = operand[:, lower_col:upper_col]
        if transposed:
            product = lax.dot_general(
                bands[nested],
                block_part,
                (((0,), (0,)), ((), ())),
                preferred_element_type=jnp.float32,
            )
        else:
            product = jnp.dot(bands[nested], block_part, preferred_element_type=jnp.float32)
        pieces.append(product)
        lower_col = upper_col
    return jnp.concatenate(pieces, axis=1)


Q_AXES = ("dp_0", "dp_1")
D_AXES = ("dp_2", "dp_3", "rep")


def on_device(queries, documents, partner):
    own_rows = queries.shape[0]
    uppers = width_list(queries.shape[1])
    rows = lax.all_gather(queries, Q_AXES, axis=0, tiled=True)
    row_partner = lax.all_gather(partner, Q_AXES, axis=0, tiled=True)
    docs = lax.all_gather(documents, D_AXES, axis=0, tiled=True)
    x_size, core_size, rep_size = [lax.axis_size(name) for name in D_AXES]
    block = lax.axis_index(Q_AXES)
    shards = block * (x_size * core_size * rep_size)
    col_ids = shards * own_rows + jnp.arange(docs.shape[0], dtype=jnp.int32)
    target = (row_partner[:, None] == col_ids[None, :]).astype(jnp.float32)
    logit_list = scores(rows, docs)
    row_peaks = jnp.stack([jnp.max(logits, axis=1) for logits in logit_list])
    masses = jnp.stack(
        [
            jnp.sum(jnp.exp(logits - row_peaks[nested][:, None]), axis=1)
            for nested, logits in enumerate(logit_list)
        ]
    )
    parts = lax.all_gather(row_peaks + jnp.log(masses), Q_AXES, axis=0)
    peak = jnp.max(parts, axis=0)
    totals = peak + jnp.log(jnp.sum(jnp.exp(parts - peak[None]), axis=0))
    bands = band_sums(
        logit_list, [totals[nested][:, None] for nested in range(len(uppers))], target, uppers
    )
    grad_documents = lax.psum_scatter(
        spread(bands, rows, uppers, True), D_AXES, scatter_dimension=0, tiled=True
    )
    grad_queries = lax.psum_scatter(
        spread(bands, docs, uppers, False), Q_AXES, scatter_dimension=0, tiled=True
    )
    return (grad_queries, grad_documents)


def solution(mesh):
    finer = Mesh(
        mesh.devices.reshape(4, 2, 4, 2, mesh.shape["rep"]), ("dp_0", "dp_1", "dp_2", "dp_3", "rep")
    )
    placed = (P(DP_REP, None), P(DP_REP, None), P(DP_REP))
    return jax.shard_map(
        on_device,
        mesh=finer,
        in_specs=placed,
        out_specs=(P(DP_REP, None), P(DP_REP, None)),
        check_vma=False,
    )
```

```python
import functools
import jax
import jax.numpy as jnp
from jax import lax
from jax.experimental import pallas as pl
from jax.experimental.pallas import tpu as pltpu
from jax.sharding import Mesh
from jax.sharding import PartitionSpec as P

WIDTHS = 9
logit_gain = 3.0


def contract(first_op, second_op):
    return lax.dot_general(
        first_op, second_op, (((1,), (1,)), ((), ())), preferred_element_type=jnp.float32
    )


def width_list(feature_dim):
    return [feature_dim >> WIDTHS - 1 - nested for nested in range(WIDTHS)]


def scores(first_op, second_op):
    uppers = width_list(first_op.shape[1])
    result = []
    running = jnp.zeros((first_op.shape[0], second_op.shape[0]), jnp.float32)
    lower_col = 0
    for upper_col in uppers:
        running = running + contract(
            first_op[:, lower_col:upper_col], second_op[:, lower_col:upper_col]
        )
        result.append(running * (logit_gain * upper_col ** (-0.5)))
        lower_col = upper_col
    return result


def band_sums(logit_list, total_list, target, uppers):
    bands = [None] * len(uppers)
    running = None
    for nested in reversed(range(len(uppers))):
        scale = logit_gain * uppers[nested] ** (-0.5)
        weight = (jnp.exp(logit_list[nested] - total_list[nested]) - target) * scale
        running = weight if running is None else running + weight
        bands[nested] = running.astype(jnp.bfloat16)
    return bands


def spread(bands, operand, uppers, transposed):
    pieces = []
    lower_col = 0
    for nested, upper_col in enumerate(uppers):
        block_part = operand[:, lower_col:upper_col]
        if transposed:
            product = lax.dot_general(
                bands[nested],
                block_part,
                (((0,), (0,)), ((), ())),
                preferred_element_type=jnp.float32,
            )
        else:
            product = jnp.dot(bands[nested], block_part, preferred_element_type=jnp.float32)
        pieces.append(product)
        lower_col = upper_col
    return jnp.concatenate(pieces, axis=1)


AXES = ("y", "zl", "x", "core", "zh")
MESH = pl.DeviceIdType.MESH
VMEM = pl.BlockSpec(memory_space=pltpu.VMEM)


def neighbours(axis):
    size = lax.axis_size(axis)
    me = lax.axis_index(axis)
    up = {axis: lax.rem(me + 1, size)}
    down = {axis: lax.rem(me + size - 1, size)}
    pair = {"zl": 1 - lax.axis_index("zl")}
    if axis == "x":
        pair["zh"] = 1 - lax.axis_index("zh")
    return up, down, pair


def meet(devices):
    barrier = pltpu.get_barrier_semaphore()
    for device in devices:
        pl.semaphore_signal(barrier, inc=1, device_id=device, device_id_type=MESH)
    pl.semaphore_wait(barrier, len(devices))


def gather_kernel(q_ref, d_ref, rows_ref, docs_ref, sent, landed):
    own = q_ref.shape[0]
    half = own // 2
    sibling = {"core": 1 - lax.axis_index("core")}
    y_up, y_down, y_pair = neighbours("y")
    x_up, x_down, x_pair = neighbours("x")
    meet((y_up, y_down, y_pair, x_up, x_down, x_pair, sibling))
    started = []
    across = []

    def send(src, dst, number, device):
        copy = pltpu.make_async_remote_copy(
            src_ref=src,
            dst_ref=dst,
            send_sem=sent.at[number],
            recv_sem=landed.at[number],
            device_id=device,
            device_id_type=MESH,
        )
        copy.start()
        started.append(copy)
        return copy

    def q_slot(step, pair, lo=0, count=own):
        return rows_ref.at[pl.ds((step * 2 + pair) * own + lo, count), :]

    def d_slot(step, pair, other=0, lo=0, count=own):
        return docs_ref.at[pl.ds(((step * 2 + pair) * 2 + other) * own + lo, count), :]

    lanes = (
        (q_ref, q_slot, y_up, y_down, y_pair, 0),
        (d_ref, d_slot, x_up, x_down, x_pair, 9),
    )
    first = []
    for src, slot, up, down, pair, base in lanes:
        first.append(
            (
                send(src, slot(0, 1), base, pair),
                send(src, slot(3, 0), base + 1, up),
                send(src, slot(1, 0), base + 2, down),
            )
        )
    across.append(send(d_ref, d_slot(0, 0, 1), 18, sibling))
    rows_ref[pl.ds(0, own), :] = q_ref[...]
    docs_ref[pl.ds(0, own), :] = d_ref[...]

    second = []
    for (src, slot, up, down, pair, base), copies in zip(lanes, first):
        copies[0].wait_recv()
        second.append(
            (
                send(slot(0, 1), slot(3, 1), base + 3, up),
                send(slot(0, 1), slot(1, 1), base + 4, down),
            )
        )
    across.append(send(d_slot(0, 1), d_slot(0, 1, 1), 19, sibling))
    far = []
    for (src, slot, up, down, pair, base), copies in zip(lanes, first):
        copies[1].wait_recv()
        far.append(send(slot(3, 0, lo=0, count=half), slot(2, 0, lo=0, count=half), base + 5, up))
        copies[2].wait_recv()
        far.append(
            send(slot(1, 0, lo=half, count=half), slot(2, 0, lo=half, count=half), base + 6, down)
        )
    across.append(send(d_slot(3, 0), d_slot(3, 0, 1), 20, sibling))
    across.append(send(d_slot(1, 0), d_slot(1, 0, 1), 21, sibling))
    for (src, slot, up, down, pair, base), copies in zip(lanes, second):
        copies[0].wait_recv()
        far.append(send(slot(3, 1, lo=0, count=half), slot(2, 1, lo=0, count=half), base + 7, up))
        copies[1].wait_recv()
        far.append(
            send(slot(1, 1, lo=half, count=half), slot(2, 1, lo=half, count=half), base + 8, down)
        )
    across.append(send(d_slot(3, 1), d_slot(3, 1, 1), 22, sibling))
    across.append(send(d_slot(1, 1), d_slot(1, 1, 1), 23, sibling))
    for copy in far:
        copy.wait_recv()
    across.append(send(d_slot(2, 0), d_slot(2, 0, 1), 24, sibling))
    across.append(send(d_slot(2, 1), d_slot(2, 1, 1), 25, sibling))
    for copy in across:
        copy.wait_recv()
    for copy in started:
        copy.wait_send()


def gather(queries, documents):
    own, wide = queries.shape
    return pl.pallas_call(
        gather_kernel,
        out_shape=(
            jax.ShapeDtypeStruct((8 * own, wide), queries.dtype),
            jax.ShapeDtypeStruct((16 * own, documents.shape[1]), documents.dtype),
        ),
        in_specs=[VMEM] * 2,
        out_specs=(VMEM, VMEM),
        scratch_shapes=[pltpu.SemaphoreType.DMA((26,)), pltpu.SemaphoreType.DMA((26,))],
        compiler_params=pltpu.CompilerParams(collective_id=0, has_side_effects=True),
        name="gather",
    )(queries, documents)


def reduce_kernel(pq_ref, pd_ref, gq_ref, gd_ref, sib, far_s, near_s, far_r, near_r, pair_s, pair_r, sent, landed):
    own = gq_ref.shape[0]
    half = own // 2
    sibling = {"core": 1 - lax.axis_index("core")}
    y_up, y_down, y_pair = neighbours("y")
    x_up, x_down, x_pair = neighbours("x")
    meet((y_up, y_down, y_pair, x_up, x_down, x_pair, sibling))
    started = []

    def send(src, dst, number, device):
        copy = pltpu.make_async_remote_copy(
            src_ref=src,
            dst_ref=dst,
            send_sem=sent.at[number],
            recv_sem=landed.at[number],
            device_id=device,
            device_id_type=MESH,
        )
        copy.start()
        started.append(copy)
        return copy

    def q_part(step, pair, lo=0, count=own):
        return pq_ref[pl.ds((step * 2 + pair) * own + lo, count), :]

    across = {}
    for place, (step, pair) in enumerate(
        ((2, 1), (2, 0), (1, 1), (3, 1), (1, 0), (3, 0), (0, 1), (0, 0))
    ):
        src = pd_ref.at[pl.ds(((step * 2 + pair) * 2 + 1) * own, own), :]
        across[step, pair] = send(src, sib.at[step * 2 + pair], 22 + place, sibling)

    def d_part(step, pair, lo=0, count=own):
        mine = pd_ref[pl.ds((step * 2 + pair) * 2 * own + lo, count), :]
        return mine + sib[step * 2 + pair, pl.ds(lo, count), :]

    lanes = ((q_part, y_up, y_down, y_pair), (d_part, x_up, x_down, x_pair))
    far = {}
    for pair in (1, 0):
        for side, (part, up, down, _) in enumerate(lanes):
            if side == 1:
                across[2, pair].wait_recv()
            far_s[side, pair] = part(2, pair).astype(jnp.bfloat16)
            for way, device in ((0, up), (1, down)):
                rows = pl.ds(way * half, half)
                far[side, pair, way] = send(
                    far_s.at[side, pair, rows],
                    far_r.at[side, pair, rows],
                    (side * 2 + pair) * 2 + way,
                    device,
                )
    near = {}
    for pair in (1, 0):
        for side, (part, up, down, _) in enumerate(lanes):
            for way, device, step in ((0, up, 1), (1, down, 3)):
                if side == 1:
                    across[step, pair].wait_recv()
                far[side, pair, way].wait_recv()
                lo = way * half
                more = half - lo
                near_s[side, pair, way, pl.ds(lo, half), :] = (
                    part(step, pair, lo, half)
                    + far_r[side, pair, pl.ds(lo, half), :].astype(jnp.float32)
                ).astype(jnp.bfloat16)
                near_s[side, pair, way, pl.ds(more, half), :] = part(
                    step, pair, more, half
                ).astype(jnp.bfloat16)
                near[side, pair, way] = send(
                    near_s.at[side, pair, way],
                    near_r.at[side, pair, way],
                    8 + (side * 2 + pair) * 2 + way,
                    device,
                )

    def total(side, pair, part):
        if side == 1:
            across[0, pair].wait_recv()
        near[side, pair, 0].wait_recv()
        near[side, pair, 1].wait_recv()
        return (
            part(0, pair)
            + near_r[side, pair, 0].astype(jnp.float32)
            + near_r[side, pair, 1].astype(jnp.float32)
        )

    last = []
    for side, (part, _, _, device) in enumerate(lanes):
        pair_s[side] = total(side, 1, part).astype(jnp.bfloat16)
        last.append(send(pair_s.at[side], pair_r.at[side], 16 + side, device))
    for side, (part, _, _, _) in enumerate(lanes):
        out = (gq_ref, gd_ref)[side]
        out[...] = total(side, 0, part)
    for side in range(2):
        out = (gq_ref, gd_ref)[side]
        last[side].wait_recv()
        out[...] = out[...] + pair_r[side].astype(jnp.float32)
    for copy in started:
        copy.wait_send()


def reduce(part_queries, part_documents):
    own = part_queries.shape[0] // 8
    dim = part_queries.shape[1]
    piece = jax.ShapeDtypeStruct((own, dim), jnp.float32)
    wire = jnp.bfloat16
    return pl.pallas_call(
        reduce_kernel,
        out_shape=(piece, piece),
        in_specs=[VMEM] * 2,
        out_specs=(VMEM, VMEM),
        scratch_shapes=[
            pltpu.VMEM((8, own, dim), jnp.float32),
            pltpu.VMEM((2, 2, own, dim), wire),
            pltpu.VMEM((2, 2, 2, own, dim), wire),
            pltpu.VMEM((2, 2, own, dim), wire),
            pltpu.VMEM((2, 2, 2, own, dim), wire),
            pltpu.VMEM((2, own, dim), wire),
            pltpu.VMEM((2, own, dim), wire),
            pltpu.SemaphoreType.DMA((30,)),
            pltpu.SemaphoreType.DMA((30,)),
        ],
        compiler_params=pltpu.CompilerParams(
            collective_id=1, has_side_effects=True, vmem_limit_bytes=60 * 2**20
        ),
        name="reduce",
    )(part_queries, part_documents)


def totals_kernel(lse_ref, out_ref, parts, sent, landed):
    chips = lax.axis_size("y")
    y = lax.axis_index("y")
    zl = lax.axis_index("zl")
    peers = []
    for step in range(chips):
        for pair in range(2):
            if step or pair:
                peers.append(
                    (step, pair, {"y": lax.rem(y + step, chips), "zl": lax.rem(zl + pair, 2)})
                )
    meet([device for _, _, device in peers])
    copies = []
    for number, (step, pair, device) in enumerate(peers):
        back = (chips - step) % chips
        copy = pltpu.make_async_remote_copy(
            src_ref=lse_ref,
            dst_ref=parts.at[back * 2 + pair],
            send_sem=sent.at[number],
            recv_sem=landed.at[back * 2 + pair],
            device_id=device,
            device_id_type=MESH,
        )
        copy.start()
        copies.append(copy)
    mine = lse_ref[...]
    for copy in copies:
        copy.wait()
    group = mine.shape[1] // chips

    def aligned(step, pair, place):
        if step == 0 and pair == 0:
            return mine[:, place * group : (place + 1) * group]
        at = (place - step) % chips * group
        piece = parts[step * 2 + pair, :, at : at + group]
        return pltpu.roll(piece, group // 2, 1) if pair else piece

    for place in range(chips):
        pieces = [aligned(step, pair, place) for step in range(chips) for pair in range(2)]
        peak = functools.reduce(jnp.maximum, pieces)
        mass = sum(jnp.exp(piece - peak) for piece in pieces)
        out_ref[:, place * group : (place + 1) * group] = peak + jnp.log(mass)


def combined_totals(lse):
    return pl.pallas_call(
        totals_kernel,
        out_shape=jax.ShapeDtypeStruct(lse.shape, jnp.float32),
        in_specs=[VMEM],
        out_specs=VMEM,
        scratch_shapes=[
            pltpu.VMEM((8, *lse.shape), jnp.float32),
            pltpu.SemaphoreType.DMA((8,)),
            pltpu.SemaphoreType.DMA((8,)),
        ],
        compiler_params=pltpu.CompilerParams(collective_id=2, has_side_effects=True),
        name="totals",
    )(lse)


def row_ids(own):
    y, zl, x, core, zh = [lax.axis_index(axis) for axis in AXES]
    chips = lax.axis_size("x")
    ids = []
    for step in range(chips):
        for pair in range(2):
            for other in range(2):
                there_x = lax.rem(x + step, chips)
                there_zl = lax.rem(zl + pair, 2)
                there_zh = lax.rem(zh + pair, 2)
                there_core = lax.rem(core + other, 2)
                chip = (y * 2 + there_zl) * chips + there_x
                shard = (chip * 2 + there_core) * 2 + there_zh
                ids.append(shard * own + jnp.arange(own, dtype=jnp.int32))
    return jnp.concatenate(ids)


def on_device(queries, documents, partner):
    own, dim = queries.shape
    uppers = width_list(dim)
    index = partner.astype(jnp.float32)
    high = jnp.floor(index / 128.0)
    low = index - 128.0 * high
    lane = jnp.arange(128)[None]
    extra = jnp.where(lane == 0, high[:, None], jnp.where(lane == 1, low[:, None], 0.0))
    rows, docs = gather(jnp.concatenate([queries, extra.astype(jnp.bfloat16)], axis=1), documents)
    marks = rows[:, dim : dim + 2].astype(jnp.float32)
    row_partner = (marks[:, 0] * 128.0 + marks[:, 1]).astype(jnp.int32)
    rows = rows[:, :dim]
    target = (row_partner[:, None] == row_ids(own)[None, :]).astype(jnp.float32)
    logit_list = scores(rows, docs)
    row_peaks = jnp.stack([jnp.max(logits, axis=1) for logits in logit_list])
    masses = jnp.stack(
        [
            jnp.sum(jnp.exp(logits - row_peaks[nested][:, None]), axis=1)
            for nested, logits in enumerate(logit_list)
        ]
    )
    lse = jnp.pad(row_peaks + jnp.log(masses), ((0, 16 - WIDTHS), (0, 0)))
    totals = combined_totals(lse)
    bands = band_sums(
        logit_list, [totals[nested][:, None] for nested in range(len(uppers))], target, uppers
    )
    return reduce(spread(bands, docs, uppers, False), spread(bands, rows, uppers, True))


def solution(mesh):
    finer = Mesh(mesh.devices.reshape(4, 2, 4, 2, mesh.shape["rep"]), AXES)
    placed = (P(AXES, None), P(AXES, None), P(AXES))
    return jax.shard_map(
        on_device,
        mesh=finer,
        in_specs=placed,
        out_specs=(P(AXES, None), P(AXES, None)),
        check_vma=False,
    )
```

```python
import functools
import jax
import jax.numpy as jnp
from jax import lax
from jax.experimental import pallas as pl
from jax.experimental.pallas import tpu as pltpu
from jax.sharding import Mesh
from jax.sharding import PartitionSpec as P

WIDTHS = 9
LOG2_E = 1.4426950408889634
logit_gain = 3.0
AXES = ("y", "zl", "x", "core", "zh")
MESH = pl.DeviceIdType.MESH
VMEM = pl.BlockSpec(memory_space=pltpu.VMEM)


def neighbours(axis):
    size = lax.axis_size(axis)
    me = lax.axis_index(axis)
    up = {axis: lax.rem(me + 1, size)}
    down = {axis: lax.rem(me + size - 1, size)}
    pair = {"zl": 1 - lax.axis_index("zl")}
    if axis == "x":
        pair["zh"] = 1 - lax.axis_index("zh")
    return up, down, pair


def meet(devices):
    barrier = pltpu.get_barrier_semaphore()
    for device in devices:
        pl.semaphore_signal(barrier, inc=1, device_id=device, device_id_type=MESH)
    pl.semaphore_wait(barrier, len(devices))


def gather_kernel(q_ref, d_ref, rows_ref, docs_ref, sent, landed):
    own = q_ref.shape[0]
    half = own // 2
    sibling = {"core": 1 - lax.axis_index("core")}
    y_up, y_down, y_pair = neighbours("y")
    x_up, x_down, x_pair = neighbours("x")
    meet((y_up, y_down, y_pair, x_up, x_down, x_pair, sibling))
    started = []
    across = []

    def send(src, dst, number, device):
        copy = pltpu.make_async_remote_copy(
            src_ref=src,
            dst_ref=dst,
            send_sem=sent.at[number],
            recv_sem=landed.at[number],
            device_id=device,
            device_id_type=MESH,
        )
        copy.start()
        started.append(copy)
        return copy

    def q_slot(step, pair, lo=0, count=own):
        return rows_ref.at[pl.ds((step * 2 + pair) * own + lo, count), :]

    def d_slot(step, pair, other=0, lo=0, count=own):
        return docs_ref.at[pl.ds(((step * 2 + pair) * 2 + other) * own + lo, count), :]

    lanes = (
        (q_ref, q_slot, y_up, y_down, y_pair, 0),
        (d_ref, d_slot, x_up, x_down, x_pair, 9),
    )
    first = []
    for src, slot, up, down, pair, base in lanes:
        first.append(
            (
                send(src, slot(0, 1), base, pair),
                send(src, slot(3, 0), base + 1, up),
                send(src, slot(1, 0), base + 2, down),
            )
        )
    across.append(send(d_ref, d_slot(0, 0, 1), 18, sibling))
    rows_ref[pl.ds(0, own), :] = q_ref[...]
    docs_ref[pl.ds(0, own), :] = d_ref[...]

    second = []
    for (src, slot, up, down, pair, base), copies in zip(lanes, first):
        copies[0].wait_recv()
        second.append(
            (
                send(slot(0, 1), slot(3, 1), base + 3, up),
                send(slot(0, 1), slot(1, 1), base + 4, down),
            )
        )
    across.append(send(d_slot(0, 1), d_slot(0, 1, 1), 19, sibling))
    far = []
    for (src, slot, up, down, pair, base), copies in zip(lanes, first):
        copies[1].wait_recv()
        far.append(send(slot(3, 0, lo=0, count=half), slot(2, 0, lo=0, count=half), base + 5, up))
        copies[2].wait_recv()
        far.append(
            send(slot(1, 0, lo=half, count=half), slot(2, 0, lo=half, count=half), base + 6, down)
        )
    across.append(send(d_slot(3, 0), d_slot(3, 0, 1), 20, sibling))
    across.append(send(d_slot(1, 0), d_slot(1, 0, 1), 21, sibling))
    for (src, slot, up, down, pair, base), copies in zip(lanes, second):
        copies[0].wait_recv()
        far.append(send(slot(3, 1, lo=0, count=half), slot(2, 1, lo=0, count=half), base + 7, up))
        copies[1].wait_recv()
        far.append(
            send(slot(1, 1, lo=half, count=half), slot(2, 1, lo=half, count=half), base + 8, down)
        )
    across.append(send(d_slot(3, 1), d_slot(3, 1, 1), 22, sibling))
    across.append(send(d_slot(1, 1), d_slot(1, 1, 1), 23, sibling))
    for copy in far:
        copy.wait_recv()
    across.append(send(d_slot(2, 0), d_slot(2, 0, 1), 24, sibling))
    across.append(send(d_slot(2, 1), d_slot(2, 1, 1), 25, sibling))
    for copy in across:
        copy.wait_recv()
    for copy in started:
        copy.wait_send()


def gather(queries, documents):
    own, wide = queries.shape
    return pl.pallas_call(
        gather_kernel,
        out_shape=(
            jax.ShapeDtypeStruct((8 * own, wide), queries.dtype),
            jax.ShapeDtypeStruct((16 * own, documents.shape[1]), documents.dtype),
        ),
        in_specs=[VMEM] * 2,
        out_specs=(VMEM, VMEM),
        scratch_shapes=[pltpu.SemaphoreType.DMA((26,)), pltpu.SemaphoreType.DMA((26,))],
        compiler_params=pltpu.CompilerParams(collective_id=0, has_side_effects=True),
        name="gather",
    )(queries, documents)


def contract(first_op, second_op, first_dim, second_dim):
    return lax.dot_general(
        first_op,
        second_op,
        (((first_dim,), (second_dim,)), ((), ())),
        preferred_element_type=jnp.float32,
    )


def width_list(feature_dim):
    return [feature_dim >> WIDTHS - 1 - nested for nested in range(WIDTHS)]


def exchange_totals(lse, parts, total, sent, landed):
    chips = lax.axis_size("y")
    copies = []
    for number, (step, pair, device) in enumerate(row_peers()):
        back = (chips - step) % chips
        copy = pltpu.make_async_remote_copy(
            src_ref=lse,
            dst_ref=parts.at[back * 2 + pair],
            send_sem=sent.at[number],
            recv_sem=landed.at[back * 2 + pair],
            device_id=device,
            device_id_type=MESH,
        )
        copy.start()
        copies.append(copy)
    for copy in copies:
        copy.wait()
    mine = lse[...]
    group = mine.shape[1] // chips

    def aligned(step, pair, place):
        if step == 0 and pair == 0:
            return mine[:, place * group : (place + 1) * group]
        at = (place - step) % chips * group
        piece = parts[step * 2 + pair, :, at : at + group]
        return pltpu.roll(piece, group // 2, 1) if pair else piece

    for place in range(chips):
        pieces = [aligned(step, pair, place) for step in range(chips) for pair in range(2)]
        peak = functools.reduce(jnp.maximum, pieces)
        mass = sum(jnp.exp(piece - peak) for piece in pieces)
        total[:, place * group : (place + 1) * group] = peak + jnp.log(mass)


def row_peers():
    chips = lax.axis_size("y")
    y = lax.axis_index("y")
    zl = lax.axis_index("zl")
    return [
        (step, pair, {"y": lax.rem(y + step, chips), "zl": lax.rem(zl + pair, 2)})
        for step in range(chips)
        for pair in range(2)
        if step or pair
    ]


def first_id(place, own):
    y, zl, x, core, zh = [lax.axis_index(axis) for axis in AXES]
    chips = lax.axis_size("x")
    step, pair, other = place // 4, lax.rem(place // 2, 2), lax.rem(place, 2)
    chip = (y * 2 + lax.rem(zl + pair, 2)) * chips + lax.rem(x + step, chips)
    return ((chip * 2 + lax.rem(core + other, 2)) * 2 + lax.rem(zh + pair, 2)) * own


def middle_kernel(
    rows_ref, docs_ref, pq_ref, pd_ref, logits, bands, peaks, lse, parts, total, partner, sent, landed
):
    count, dim = docs_ref.shape
    width = rows_ref.shape[0]
    own = count // 16
    uppers = width_list(dim)
    lowers = [0] + uppers[:-1]
    scales = [logit_gain * upper ** (-0.5) for upper in uppers]
    narrow = 256
    few = uppers.index(narrow) + 1
    meet([device for _, _, device in row_peers()])

    marks = jnp.transpose(rows_ref[:, dim : dim + 128].astype(jnp.float32))
    partner[...] = (marks[0:1] * 128.0 + marks[1:2]).astype(jnp.int32)

    tall = count // 2

    def score_block(block, carry):
        at = pl.ds(pl.multiple_of(block * tall, tall), tall)
        lane = lax.broadcasted_iota(jnp.int32, (tall, narrow), 1)
        head = docs_ref[at, :narrow]
        for nested in range(few):
            cut = jnp.where(lane < uppers[nested], head, jnp.zeros_like(head))
            logits[nested, at, :] = contract(cut, rows_ref[:, :narrow], 1, 1)
        for nested in range(few, WIDTHS):
            cols = slice(lowers[nested], uppers[nested])
            logits[nested, at, :] = logits[nested - 1, at, :] + contract(
                docs_ref[at, cols], rows_ref[:, cols], 1, 1
            )
        return carry

    lax.fori_loop(0, 2, score_block, 0)

    lse[...] = jnp.zeros_like(lse)
    step_rows = 64
    for nested in range(WIDTHS):

        def peak_block(block, best):
            at = pl.ds(pl.multiple_of(block * step_rows, step_rows), step_rows)
            piece = logits[nested, at, :].reshape(step_rows // 8, 8, width)
            return jnp.maximum(best, jnp.max(piece, axis=0))

        best = lax.fori_loop(
            0, count // step_rows, peak_block, jnp.full((8, width), -jnp.inf, jnp.float32)
        )
        peak = jnp.max(best, axis=0, keepdims=True)

        def mass_block(block, mass):
            at = pl.ds(pl.multiple_of(block * step_rows, step_rows), step_rows)
            piece = jnp.exp2((logits[nested, at, :] - peak) * (scales[nested] * LOG2_E))
            logits[nested, at, :] = piece
            return mass + jnp.sum(piece.reshape(step_rows // 8, 8, width), axis=0)

        mass = lax.fori_loop(0, count // step_rows, mass_block, jnp.zeros((8, width), jnp.float32))
        mass = jnp.sum(mass, axis=0, keepdims=True)
        peaks[nested : nested + 1, :] = peak * scales[nested]
        lse[nested : nested + 1, :] = peak * scales[nested] + jnp.log(mass)

    exchange_totals(lse, parts, total, sent, landed)

    for nested in range(WIDTHS):
        row = slice(nested, nested + 1)
        peaks[row, :] = jnp.exp(peaks[row, :] - total[row, :]) * scales[nested]
    short = 32

    def band_block(block, carry):
        at = pl.ds(pl.multiple_of(block * short, short), short)
        per = own // short
        base = first_id(block // per, own) + lax.rem(block, per) * short
        ids = base + lax.broadcasted_iota(jnp.int32, (short, width), 0)
        hit = ids == partner[...]
        running = jnp.zeros((short, width), jnp.float32)
        gone = 0.0
        for nested in reversed(range(WIDTHS)):
            running = running + logits[nested, at, :] * peaks[nested : nested + 1, :]
            gone += scales[nested]
            band = running - jnp.where(hit, gone, 0.0)
            bands[at, nested * width : (nested + 1) * width] = band.astype(jnp.bfloat16)
        return carry

    lax.fori_loop(0, count // short, band_block, 0)

    piece = 256

    def doc_block(block, carry):
        at = pl.ds(pl.multiple_of(block * piece, piece), piece)
        lane = lax.broadcasted_iota(jnp.int32, (piece, narrow), 1)
        head = None
        for nested in range(WIDTHS):
            cols = slice(0, narrow) if nested < few else slice(lowers[nested], uppers[nested])
            part = contract(
                bands[at, nested * width : (nested + 1) * width], rows_ref[:, cols], 1, 0
            )
            if nested < few:
                head = part if head is None else jnp.where(lane < lowers[nested], head, part)
                part = head
            if nested >= few - 1:
                pd_ref[at, cols] = part
        return carry

    lax.fori_loop(0, count // piece, doc_block, 0)

    def row_block(block, carry):
        at = pl.ds(pl.multiple_of(block * piece, piece), piece)
        lane = lax.broadcasted_iota(jnp.int32, (piece, narrow), 1)
        head = None
        for nested in range(WIDTHS):
            cols = slice(0, narrow) if nested < few else slice(lowers[nested], uppers[nested])
            start = pl.multiple_of(nested * width + block * piece, piece)
            part = contract(bands[:, pl.ds(start, piece)], docs_ref[:, cols], 0, 0)
            if nested < few:
                head = part if head is None else jnp.where(lane < lowers[nested], head, part)
                part = head
            if nested >= few - 1:
                pq_ref[at, cols] = part
        return carry

    lax.fori_loop(0, width // piece, row_block, 0)


def middle(rows, docs):
    count, dim = docs.shape
    width = rows.shape[0]
    return pl.pallas_call(
        middle_kernel,
        out_shape=(
            jax.ShapeDtypeStruct((width, dim), jnp.float32),
            jax.ShapeDtypeStruct((count, dim), jnp.float32),
        ),
        in_specs=[VMEM] * 2,
        out_specs=(VMEM, VMEM),
        scratch_shapes=[
            pltpu.VMEM((WIDTHS, count, width), jnp.float32),
            pltpu.VMEM((count, WIDTHS * width), jnp.bfloat16),
            pltpu.VMEM((16, width), jnp.float32),
            pltpu.VMEM((16, width), jnp.float32),
            pltpu.VMEM((8, 16, width), jnp.float32),
            pltpu.VMEM((16, width), jnp.float32),
            pltpu.VMEM((1, width), jnp.int32),
            pltpu.SemaphoreType.DMA((8,)),
            pltpu.SemaphoreType.DMA((8,)),
        ],
        compiler_params=pltpu.CompilerParams(
            collective_id=2, has_side_effects=True, vmem_limit_bytes=60 * 2**20
        ),
        name="middle",
    )(rows, docs)


def reduce_kernel(pq_ref, pd_ref, gq_ref, gd_ref, sib, far_s, near_s, far_r, near_r, pair_s, pair_r, sent, landed):
    own = gq_ref.shape[0]
    half = own // 2
    sibling = {"core": 1 - lax.axis_index("core")}
    y_up, y_down, y_pair = neighbours("y")
    x_up, x_down, x_pair = neighbours("x")
    meet((y_up, y_down, y_pair, x_up, x_down, x_pair, sibling))
    started = []

    def send(src, dst, number, device):
        copy = pltpu.make_async_remote_copy(
            src_ref=src,
            dst_ref=dst,
            send_sem=sent.at[number],
            recv_sem=landed.at[number],
            device_id=device,
            device_id_type=MESH,
        )
        copy.start()
        started.append(copy)
        return copy

    def q_part(step, pair, lo=0, count=own):
        return pq_ref[pl.ds((step * 2 + pair) * own + lo, count), :]

    across = {}
    for place, (step, pair) in enumerate(
        ((2, 1), (2, 0), (1, 1), (3, 1), (1, 0), (3, 0), (0, 1), (0, 0))
    ):
        src = pd_ref.at[pl.ds(((step * 2 + pair) * 2 + 1) * own, own), :]
        across[step, pair] = send(src, sib.at[step * 2 + pair], 22 + place, sibling)

    def d_part(step, pair, lo=0, count=own):
        mine = pd_ref[pl.ds((step * 2 + pair) * 2 * own + lo, count), :]
        return mine + sib[step * 2 + pair, pl.ds(lo, count), :]

    lanes = ((q_part, y_up, y_down, y_pair), (d_part, x_up, x_down, x_pair))
    far = {}
    for pair in (1, 0):
        for side, (part, up, down, _) in enumerate(lanes):
            if side == 1:
                across[2, pair].wait_recv()
            far_s[side, pair] = part(2, pair).astype(jnp.bfloat16)
            for way, device in ((0, up), (1, down)):
                rows = pl.ds(way * half, half)
                far[side, pair, way] = send(
                    far_s.at[side, pair, rows],
                    far_r.at[side, pair, rows],
                    (side * 2 + pair) * 2 + way,
                    device,
                )
    near = {}
    for pair in (1, 0):
        for side, (part, up, down, _) in enumerate(lanes):
            for way, device, step in ((0, up, 1), (1, down, 3)):
                if side == 1:
                    across[step, pair].wait_recv()
                far[side, pair, way].wait_recv()
                lo = way * half
                more = half - lo
                near_s[side, pair, way, pl.ds(lo, half), :] = (
                    part(step, pair, lo, half)
                    + far_r[side, pair, pl.ds(lo, half), :].astype(jnp.float32)
                ).astype(jnp.bfloat16)
                near_s[side, pair, way, pl.ds(more, half), :] = part(
                    step, pair, more, half
                ).astype(jnp.bfloat16)
                near[side, pair, way] = send(
                    near_s.at[side, pair, way],
                    near_r.at[side, pair, way],
                    8 + (side * 2 + pair) * 2 + way,
                    device,
                )

    def total(side, pair, part):
        if side == 1:
            across[0, pair].wait_recv()
        near[side, pair, 0].wait_recv()
        near[side, pair, 1].wait_recv()
        return (
            part(0, pair)
            + near_r[side, pair, 0].astype(jnp.float32)
            + near_r[side, pair, 1].astype(jnp.float32)
        )

    last = []
    for side, (part, _, _, device) in enumerate(lanes):
        pair_s[side] = total(side, 1, part).astype(jnp.bfloat16)
        last.append(send(pair_s.at[side], pair_r.at[side], 16 + side, device))
    for side, (part, _, _, _) in enumerate(lanes):
        out = (gq_ref, gd_ref)[side]
        out[...] = total(side, 0, part)
    for side in range(2):
        out = (gq_ref, gd_ref)[side]
        last[side].wait_recv()
        out[...] = out[...] + pair_r[side].astype(jnp.float32)
    for copy in started:
        copy.wait_send()


def reduce(part_queries, part_documents):
    own = part_queries.shape[0] // 8
    dim = part_queries.shape[1]
    piece = jax.ShapeDtypeStruct((own, dim), jnp.float32)
    wire = jnp.bfloat16
    return pl.pallas_call(
        reduce_kernel,
        out_shape=(piece, piece),
        in_specs=[VMEM] * 2,
        out_specs=(VMEM, VMEM),
        scratch_shapes=[
            pltpu.VMEM((8, own, dim), jnp.float32),
            pltpu.VMEM((2, 2, own, dim), wire),
            pltpu.VMEM((2, 2, 2, own, dim), wire),
            pltpu.VMEM((2, 2, own, dim), wire),
            pltpu.VMEM((2, 2, 2, own, dim), wire),
            pltpu.VMEM((2, own, dim), wire),
            pltpu.VMEM((2, own, dim), wire),
            pltpu.SemaphoreType.DMA((30,)),
            pltpu.SemaphoreType.DMA((30,)),
        ],
        compiler_params=pltpu.CompilerParams(
            collective_id=1, has_side_effects=True, vmem_limit_bytes=60 * 2**20
        ),
        name="reduce",
    )(part_queries, part_documents)


def on_device(queries, documents, partner):
    index = partner.astype(jnp.float32)
    high = jnp.floor(index / 128.0)
    low = index - 128.0 * high
    lane = jnp.arange(128)[None]
    extra = jnp.where(lane == 0, high[:, None], jnp.where(lane == 1, low[:, None], 0.0))
    rows, docs = gather(jnp.concatenate([queries, extra.astype(jnp.bfloat16)], axis=1), documents)
    return reduce(*middle(rows, docs))


def solution(mesh):
    finer = Mesh(mesh.devices.reshape(4, 2, 4, 2, mesh.shape["rep"]), AXES)
    placed = (P(AXES, None), P(AXES, None), P(AXES))
    return jax.shard_map(
        on_device,
        mesh=finer,
        in_specs=placed,
        out_specs=(P(AXES, None), P(AXES, None)),
        check_vma=False,
    )
```

```python
import functools
import jax
import jax.numpy as jnp
from jax import lax
from jax.experimental import pallas as pl
from jax.experimental.pallas import tpu as pltpu
from jax.sharding import Mesh
from jax.sharding import PartitionSpec as P

WIDTHS = 9
LOG2_E = 1.4426950408889634
logit_gain = 3.0

AXES = ("y", "zl", "x", "core", "zh")
MESH = pl.DeviceIdType.MESH
VMEM = pl.BlockSpec(memory_space=pltpu.VMEM)


def width_list(feature_dim):
    return [feature_dim >> WIDTHS - 1 - nested for nested in range(WIDTHS)]


def contract(first_op, second_op, first_dim, second_dim):
    return lax.dot_general(
        first_op,
        second_op,
        (((first_dim,), (second_dim,)), ((), ())),
        preferred_element_type=jnp.float32,
    )


def neighbours(axis):
    size = lax.axis_size(axis)
    me = lax.axis_index(axis)
    up = {axis: lax.rem(me + 1, size)}
    down = {axis: lax.rem(me + size - 1, size)}
    pair = {"zl": 1 - lax.axis_index("zl")}
    if axis == "x":
        pair["zh"] = 1 - lax.axis_index("zh")
    return up, down, pair


def row_peers():
    chips = lax.axis_size("y")
    y = lax.axis_index("y")
    zl = lax.axis_index("zl")
    return [
        (step, pair, {"y": lax.rem(y + step, chips), "zl": lax.rem(zl + pair, 2)})
        for step in range(chips)
        for pair in range(2)
        if step or pair
    ]


def first_id(place, own):
    y, zl, x, core, zh = [lax.axis_index(axis) for axis in AXES]
    chips = lax.axis_size("x")
    step, pair, other = place // 4, lax.rem(place // 2, 2), lax.rem(place, 2)
    chip = (y * 2 + lax.rem(zl + pair, 2)) * chips + lax.rem(x + step, chips)
    return ((chip * 2 + lax.rem(core + other, 2)) * 2 + lax.rem(zh + pair, 2)) * own


def meet(devices):
    barrier = pltpu.get_barrier_semaphore()
    for device in devices:
        pl.semaphore_signal(barrier, inc=1, device_id=device, device_id_type=MESH)
    pl.semaphore_wait(barrier, len(devices))


class Sender:
    def __init__(self, sent, landed):
        self.sent, self.landed, self.started = sent, landed, []

    def __call__(self, src, dst, device, number=None, arrival=None):
        number = len(self.started)
        copy = pltpu.make_async_remote_copy(
            src_ref=src,
            dst_ref=dst,
            send_sem=self.sent.at[number],
            recv_sem=self.landed.at[number if arrival is None else arrival],
            device_id=device,
            device_id_type=MESH,
        )
        copy.start()
        self.started.append(copy)
        return copy

    def finish(self):
        for copy in self.started:
            copy.wait_send()


def gather(send, q_ref, d_ref, rows_ref, docs_ref):
    own = q_ref.shape[0]
    half = own // 2
    sibling = {"core": 1 - lax.axis_index("core")}

    def q_slot(step, pair, lo=0, count=own):
        return rows_ref.at[pl.ds((step * 2 + pair) * own + lo, count), :]

    def d_slot(step, pair, other=0, lo=0, count=own):
        return docs_ref.at[pl.ds(((step * 2 + pair) * 2 + other) * own + lo, count), :]

    lanes = ((q_ref, q_slot, *neighbours("y")), (d_ref, d_slot, *neighbours("x")))
    first = []
    for src, slot, up, down, pair in lanes:
        first.append(
            (
                send(src, slot(0, 1), pair),
                send(src, slot(3, 0), up),
                send(src, slot(1, 0), down),
            )
        )
    across = [send(d_ref, d_slot(0, 0, 1), sibling)]
    rows_ref[pl.ds(0, own), :] = q_ref[...]
    docs_ref[pl.ds(0, own), :] = d_ref[...]
    second = []
    for (src, slot, up, down, pair), copies in zip(lanes, first):
        copies[0].wait_recv()
        second.append(
            (
                send(slot(0, 1), slot(3, 1), up),
                send(slot(0, 1), slot(1, 1), down),
            )
        )
    across.append(send(d_slot(0, 1), d_slot(0, 1, 1), sibling))
    far = []
    for pair, stage in ((0, first), (1, second)):
        for (src, slot, up, down, _), copies in zip(lanes, stage):
            for copy, step, device, lo in ((copies[-2], 3, up, 0), (copies[-1], 1, down, half)):
                copy.wait_recv()
                far.append(
                    send(
                        slot(step, pair, lo=lo, count=half),
                        slot(2, pair, lo=lo, count=half),
                        device,
                    )
                )
        for step in (3, 1):
            across.append(send(d_slot(step, pair), d_slot(step, pair, 1), sibling))
    for copy in far:
        copy.wait_recv()
    for pair in range(2):
        across.append(send(d_slot(2, pair), d_slot(2, pair, 1), sibling))
    for copy in across:
        copy.wait_recv()


def exchange_totals(send, lse, parts, total):
    chips = lax.axis_size("y")
    copies = [
        send(lse, parts.at[(chips - step) % chips * 2 + pair], device)
        for step, pair, device in row_peers()
    ]
    for copy in copies:
        copy.wait_recv()
    mine = lse[...]
    group = mine.shape[1] // chips

    def aligned(step, pair, place):
        if step == 0 and pair == 0:
            return mine[:, place * group : (place + 1) * group]
        at = (place - step) % chips * group
        piece = parts[step * 2 + pair, :, at : at + group]
        return pltpu.roll(piece, group // 2, 1) if pair else piece

    for place in range(chips):
        pieces = [aligned(step, pair, place) for step in range(chips) for pair in range(2)]
        peak = functools.reduce(jnp.maximum, pieces)
        mass = sum(jnp.exp(piece - peak) for piece in pieces)
        total[:, place * group : (place + 1) * group] = peak + jnp.log(mass)


def step_kernel(
    q_ref,
    d_ref,
    p_ref,
    gq_ref,
    gd_ref,
    rows_ref,
    docs_ref,
    logits,
    bands,
    peaks,
    lse,
    parts,
    total,
    marks,
    pq_ref,
    pd_ref,
    sib,
    far_s,
    near_s,
    far_r,
    near_r,
    pair_s,
    pair_r,
    sent,
    landed,
):
    count, dim = docs_ref.shape
    width = rows_ref.shape[0]
    own = q_ref.shape[0]
    half = own // 2
    uppers = width_list(dim)
    lowers = [0] + uppers[:-1]
    scales = [logit_gain * upper ** (-0.5) for upper in uppers]
    narrow = 256
    few = uppers.index(narrow) + 1
    chips = lax.axis_size("y")
    sibling = {"core": 1 - lax.axis_index("core")}
    meet([device for _, _, device in row_peers()] + [*neighbours("x"), sibling])
    send = Sender(sent, landed)

    marked = [
        send(p_ref, marks.at[(chips - step) % chips * 2 + pair], device)
        for step, pair, device in row_peers()
    ]
    gather(send, q_ref, d_ref, rows_ref, docs_ref)

    tall = count // 2

    def score_block(block, carry):
        at = pl.ds(pl.multiple_of(block * tall, tall), tall)
        lane = lax.broadcasted_iota(jnp.int32, (tall, narrow), 1)
        head = docs_ref[at, :narrow]
        for nested in range(few):
            cut = jnp.where(lane < uppers[nested], head, jnp.zeros_like(head))
            logits[nested, at, :] = contract(cut, rows_ref[:, :narrow], 1, 1)
        for nested in range(few, WIDTHS):
            cols = slice(lowers[nested], uppers[nested])
            logits[nested, at, :] = logits[nested - 1, at, :] + contract(
                docs_ref[at, cols], rows_ref[:, cols], 1, 1
            )
        return carry

    lax.fori_loop(0, 2, score_block, 0)

    lse[...] = jnp.zeros_like(lse)
    step_rows = 64
    for nested in range(WIDTHS):

        def peak_block(block, best):
            at = pl.ds(pl.multiple_of(block * step_rows, step_rows), step_rows)
            piece = logits[nested, at, :].reshape(step_rows // 8, 8, width)
            return jnp.maximum(best, jnp.max(piece, axis=0))

        best = lax.fori_loop(
            0, count // step_rows, peak_block, jnp.full((8, width), -jnp.inf, jnp.float32)
        )
        peak = jnp.max(best, axis=0, keepdims=True)

        def mass_block(block, mass):
            at = pl.ds(pl.multiple_of(block * step_rows, step_rows), step_rows)
            piece = jnp.exp2((logits[nested, at, :] - peak) * (scales[nested] * LOG2_E))
            logits[nested, at, :] = piece
            return mass + jnp.sum(piece.reshape(step_rows // 8, 8, width), axis=0)

        mass = lax.fori_loop(0, count // step_rows, mass_block, jnp.zeros((8, width), jnp.float32))
        mass = jnp.sum(mass, axis=0, keepdims=True)
        peaks[nested : nested + 1, :] = peak * scales[nested]
        lse[nested : nested + 1, :] = peak * scales[nested] + jnp.log(mass)

    exchange_totals(send, lse, parts, total)
    for copy in marked:
        copy.wait_recv()

    for nested in range(WIDTHS):
        row = slice(nested, nested + 1)
        peaks[row, :] = jnp.exp(peaks[row, :] - total[row, :]) * scales[nested]
    side = lax.broadcasted_iota(jnp.int32, (1, 2 * own), 1)
    partner = []
    for step in range(chips):
        near_mark = p_ref[0:1, :] if step == 0 else marks[step * 2, 0:1, :]
        partner.append(jnp.where(side < own, near_mark, marks[step * 2 + 1, 0:1, :]))
    partner = jnp.concatenate(partner, axis=1)
    short = 32

    def band_block(block, carry):
        at = pl.ds(pl.multiple_of(block * short, short), short)
        per = own // short
        base = first_id(block // per, own) + lax.rem(block, per) * short
        ids = base + lax.broadcasted_iota(jnp.int32, (short, width), 0)
        hit = ids == partner
        running = jnp.zeros((short, width), jnp.float32)
        gone = 0.0
        for nested in reversed(range(WIDTHS)):
            running = running + logits[nested, at, :] * peaks[nested : nested + 1, :]
            gone += scales[nested]
            band = running - jnp.where(hit, gone, 0.0)
            bands[at, nested * width : (nested + 1) * width] = band.astype(jnp.bfloat16)
        return carry

    lax.fori_loop(0, count // short, band_block, 0)

    def bounds(nested):
        return slice(0, narrow) if nested < few else slice(lowers[nested], uppers[nested])

    def product(tall_rows, get, out_ref, at):
        lane = lax.broadcasted_iota(jnp.int32, (tall_rows, narrow), 1)
        head = None
        for nested in range(WIDTHS):
            part = get(nested, bounds(nested))
            if nested < few:
                head = part if head is None else jnp.where(lane < lowers[nested], head, part)
                part = head
            if nested >= few - 1:
                out_ref[at, bounds(nested)] = part

    across = {}

    def documents_for(step):
        piece = 4 * own
        at = slice(step * piece, (step + 1) * piece)
        product(
            piece,
            lambda nested, cols: contract(
                bands[at, nested * width : (nested + 1) * width], rows_ref[:, cols], 1, 0
            ),
            pd_ref,
            at,
        )
        for pair in (1, 0):
            theirs = pd_ref.at[pl.ds(((step * 2 + pair) * 2 + 1) * own, own), :]
            across[step, pair] = send(theirs, sib.at[step * 2 + pair], sibling)

    def queries_for(step):
        piece = 2 * own
        product(
            piece,
            lambda nested, cols: contract(
                bands[:, nested * width + step * piece : nested * width + (step + 1) * piece],
                docs_ref[:, cols],
                0,
                0,
            ),
            pq_ref,
            slice(step * piece, (step + 1) * piece),
        )

    def q_part(step, pair, lo=0, size=own):
        return pq_ref[pl.ds((step * 2 + pair) * own + lo, size), :]

    def d_part(step, pair, lo=0, size=own):
        mine = pd_ref[pl.ds((step * 2 + pair) * 2 * own + lo, size), :]
        return mine + sib[step * 2 + pair, pl.ds(lo, size), :]

    lanes = ((q_part, *neighbours("y")), (d_part, *neighbours("x")))
    far = {}
    near = {}

    def send_far(which, pair):
        part, up, down, _ = lanes[which]
        far_s[which, pair] = part(2, pair).astype(jnp.bfloat16)
        for way, device in ((0, up), (1, down)):
            piece = pl.ds(way * half, half)
            far[which, pair, way] = send(
                far_s.at[which, pair, piece], far_r.at[which, pair, piece], device
            )

    def send_near(which, pair):
        part, up, down, _ = lanes[which]
        for way, device, step in ((0, up, 1), (1, down, 3)):
            if which == 1:
                across[step, pair].wait_recv()
            far[which, pair, way].wait_recv()
            lo = way * half
            more = half - lo
            near_s[which, pair, way, pl.ds(lo, half), :] = (
                part(step, pair, lo, half)
                + far_r[which, pair, pl.ds(lo, half), :].astype(jnp.float32)
            ).astype(jnp.bfloat16)
            near_s[which, pair, way, pl.ds(more, half), :] = part(step, pair, more, half).astype(
                jnp.bfloat16
            )
            near[which, pair, way] = send(
                near_s.at[which, pair, way], near_r.at[which, pair, way], device
            )

    def arrived(which, pair):
        part = lanes[which][0]
        if which == 1:
            across[0, pair].wait_recv()
        near[which, pair, 0].wait_recv()
        near[which, pair, 1].wait_recv()
        return (
            part(0, pair)
            + near_r[which, pair, 0].astype(jnp.float32)
            + near_r[which, pair, 1].astype(jnp.float32)
        )

    documents_for(2)
    queries_for(2)
    send_far(0, 1)
    send_far(0, 0)
    for pair in (1, 0):
        across[2, pair].wait_recv()
        send_far(1, pair)
    documents_for(1)
    documents_for(3)
    queries_for(1)
    queries_for(3)
    for pair in (1, 0):
        send_near(0, pair)
        send_near(1, pair)
    documents_for(0)
    queries_for(0)
    last = []
    for which in range(2):
        pair_s[which] = arrived(which, 1).astype(jnp.bfloat16)
        last.append(send(pair_s.at[which], pair_r.at[which], lanes[which][3]))
    outs = (gq_ref, gd_ref)
    for which in range(2):
        outs[which][...] = arrived(which, 0)
    for which in range(2):
        last[which].wait_recv()
        outs[which][...] = outs[which][...] + pair_r[which].astype(jnp.float32)
    send.finish()


def on_device(queries, documents, partner):
    own, dim = queries.shape
    width, count = 8 * own, 16 * own
    piece = jax.ShapeDtypeStruct((own, dim), jnp.float32)
    wire = jnp.bfloat16
    copies = 7 + 26 + 7 + 30
    return pl.pallas_call(
        step_kernel,
        out_shape=(piece, piece),
        in_specs=[VMEM] * 3,
        out_specs=(VMEM, VMEM),
        scratch_shapes=[
            pltpu.VMEM((width, dim), wire),
            pltpu.VMEM((count, dim), wire),
            pltpu.VMEM((WIDTHS, count, width), jnp.float32),
            pltpu.VMEM((count, WIDTHS * width), wire),
            pltpu.VMEM((16, width), jnp.float32),
            pltpu.VMEM((16, width), jnp.float32),
            pltpu.VMEM((8, 16, width), jnp.float32),
            pltpu.VMEM((16, width), jnp.float32),
            pltpu.VMEM((8, 8, 2 * own), jnp.int32),
            pltpu.VMEM((width, dim), jnp.float32),
            pltpu.VMEM((count, dim), jnp.float32),
            pltpu.VMEM((8, own, dim), jnp.float32),
            pltpu.VMEM((2, 2, own, dim), wire),
            pltpu.VMEM((2, 2, 2, own, dim), wire),
            pltpu.VMEM((2, 2, own, dim), wire),
            pltpu.VMEM((2, 2, 2, own, dim), wire),
            pltpu.VMEM((2, own, dim), wire),
            pltpu.VMEM((2, own, dim), wire),
            pltpu.SemaphoreType.DMA((copies,)),
            pltpu.SemaphoreType.DMA((copies,)),
        ],
        compiler_params=pltpu.CompilerParams(
            collective_id=0, has_side_effects=True, vmem_limit_bytes=67043328
        ),
        name="step",
    )(queries, documents, jnp.tile(partner[None, :], (8, 2)))


def solution(mesh):
    finer = Mesh(mesh.devices.reshape(4, 2, 4, 2, mesh.shape["rep"]), AXES)
    placed = (P(AXES, None), P(AXES, None), P(AXES))
    return jax.shard_map(
        on_device,
        mesh=finer,
        in_specs=placed,
        out_specs=(P(AXES, None), P(AXES, None)),
        check_vma=False,
    )
```

```python
import functools
import jax
import jax.numpy as jnp
from jax import lax
from jax.experimental import pallas as pl
from jax.experimental.pallas import tpu as pltpu
from jax.sharding import Mesh
from jax.sharding import PartitionSpec as P

WIDTHS = 9
LOG2_E = 1.4426950408889634
logit_gain = 3.0

AXES = ("y", "zl", "x", "core", "zh")
MESH = pl.DeviceIdType.MESH
VMEM = pl.BlockSpec(memory_space=pltpu.VMEM)


def width_list(feature_dim):
    return [feature_dim >> WIDTHS - 1 - nested for nested in range(WIDTHS)]


def contract(first_op, second_op, first_dim, second_dim):
    return lax.dot_general(
        first_op,
        second_op,
        (((first_dim,), (second_dim,)), ((), ())),
        preferred_element_type=jnp.float32,
    )


def neighbours(axis):
    size = lax.axis_size(axis)
    me = lax.axis_index(axis)
    up = {axis: lax.rem(me + 1, size)}
    down = {axis: lax.rem(me + size - 1, size)}
    pair = {"zl": 1 - lax.axis_index("zl")}
    if axis == "x":
        pair["zh"] = 1 - lax.axis_index("zh")
    return up, down, pair


def row_peers():
    chips = lax.axis_size("y")
    y = lax.axis_index("y")
    zl = lax.axis_index("zl")
    return [
        (step, pair, {"y": lax.rem(y + step, chips), "zl": lax.rem(zl + pair, 2)})
        for step in range(chips)
        for pair in range(2)
        if step or pair
    ]


def place_of_row(step, pair):
    y = lax.rem(lax.axis_index("y") + step, lax.axis_size("y"))
    return y * 2 + lax.rem(lax.axis_index("zl") + pair, 2)


def place_of_doc(step, pair, other):
    x = lax.rem(lax.axis_index("x") + step, lax.axis_size("x"))
    zh = lax.rem(lax.axis_index("zh") + pair, 2)
    return (x * 2 + zh) * 2 + lax.rem(lax.axis_index("core") + other, 2)


def first_id(place, own):
    x, there, core = place // 4, lax.rem(place // 2, 2), lax.rem(place, 2)
    zl = lax.rem(lax.axis_index("zl") + lax.axis_index("zh") + there, 2)
    chip = (lax.axis_index("y") * 2 + zl) * lax.axis_size("x") + x
    return ((chip * 2 + core) * 2 + there) * own


def meet(devices):
    barrier = pltpu.get_barrier_semaphore()
    for device in devices:
        pl.semaphore_signal(barrier, inc=1, device_id=device, device_id_type=MESH)
    pl.semaphore_wait(barrier, len(devices))


class Sender:
    def __init__(self, sent, landed):
        self.sent, self.landed, self.started = sent, landed, []

    def __call__(self, src, dst, device):
        number = len(self.started)
        copy = pltpu.make_async_remote_copy(
            src_ref=src,
            dst_ref=dst,
            send_sem=self.sent.at[number],
            recv_sem=self.landed.at[number],
            device_id=device,
            device_id_type=MESH,
        )
        copy.start()
        self.started.append(copy)
        return copy

    def finish(self):
        for copy in self.started:
            copy.wait_send()


def gather(send, q_ref, d_ref, rows_ref, docs_ref):
    own = q_ref.shape[0]
    half = own // 2
    sibling = {"core": 1 - lax.axis_index("core")}

    def q_slot(step, pair, lo=0, size=own):
        start = place_of_row(step, pair) * own + lo
        return rows_ref.at[pl.ds(pl.multiple_of(start, half), size), :]

    def d_slot(step, pair, lo=0, size=own):
        start = place_of_doc(step, pair, 0) * own + lo
        return docs_ref.at[pl.ds(pl.multiple_of(start, half), size), :]

    lanes = ((q_ref, q_slot, *neighbours("y")), (d_ref, d_slot, *neighbours("x")))
    first = [
        tuple(send(src, slot(0, 0), device) for device in (pair, up, down))
        for src, slot, up, down, pair in lanes
    ]
    across = [send(d_ref, d_slot(0, 0), sibling)]
    rows_ref[pl.ds(pl.multiple_of(place_of_row(0, 0) * own, own), own), :] = q_ref[...]
    docs_ref[pl.ds(pl.multiple_of(place_of_doc(0, 0, 0) * own, own), own), :] = d_ref[...]
    second = []
    for (src, slot, up, down, _), copies in zip(lanes, first):
        copies[0].wait_recv()
        second.append(tuple(send(slot(0, 1), slot(0, 1), device) for device in (up, down)))
    across.append(send(d_slot(0, 1), d_slot(0, 1), sibling))
    far = []
    for pair, stage in ((0, first), (1, second)):
        for (src, slot, up, down, _), copies in zip(lanes, stage):
            for copy, step, device, lo in ((copies[-2], 3, up, 0), (copies[-1], 1, down, half)):
                copy.wait_recv()
                piece = slot(step, pair, lo, half)
                far.append(send(piece, piece, device))
        for step in (3, 1):
            across.append(send(d_slot(step, pair), d_slot(step, pair), sibling))
    for copy in far:
        copy.wait_recv()
    for pair in range(2):
        across.append(send(d_slot(2, pair), d_slot(2, pair), sibling))
    for copy in across:
        copy.wait_recv()


def step_kernel(
    q_ref,
    d_ref,
    p_ref,
    gq_ref,
    gd_ref,
    rows_ref,
    docs_ref,
    logits,
    bands,
    best,
    mass,
    peaks,
    lse,
    parts,
    marks,
    pq_ref,
    pd_ref,
    sib,
    far_s,
    near_s,
    far_r,
    near_r,
    pair_s,
    pair_r,
    sent,
    landed,
):
    count, dim = docs_ref.shape
    width = rows_ref.shape[0]
    own = q_ref.shape[0]
    half = own // 2
    uppers = width_list(dim)
    lowers = [0] + uppers[:-1]
    scales = [logit_gain * upper ** (-0.5) for upper in uppers]
    narrow = 256
    few = uppers.index(narrow) + 1
    chips = lax.axis_size("y")
    sibling = {"core": 1 - lax.axis_index("core")}
    meet([device for _, _, device in row_peers()] + [*neighbours("x"), sibling])
    send = Sender(sent, landed)

    marked = [send(p_ref, marks.at[place_of_row(0, 0)], device) for _, _, device in row_peers()]
    marks[place_of_row(0, 0)] = p_ref[...]
    lse[...] = jnp.zeros_like(lse)
    peaks[...] = jnp.zeros_like(peaks)
    gather(send, q_ref, d_ref, rows_ref, docs_ref)
    for copy in marked:
        copy.wait_recv()
    side = lax.broadcasted_iota(jnp.int32, (1, 2 * own), 1)
    partner = jnp.concatenate(
        [
            jnp.where(side < own, marks[2 * step, 0:1, :], marks[2 * step + 1, 0:1, :])
            for step in range(chips)
        ],
        axis=1,
    )

    turn = width // 2
    tall = count // 2

    def turn_cols(part, nested=0):
        start = nested * width + part * turn
        return slice(start, start + turn)

    def score(part):
        cols_q = turn_cols(part)
        best[...] = jnp.full(best.shape, -jnp.inf, jnp.float32)

        def keep(nested, at, value):
            logits[nested, at, cols_q] = value
            top = jnp.max(value.reshape(tall // 8, 8, turn), axis=0)
            best[nested] = jnp.maximum(best[nested], top)

        def score_block(block, carry):
            at = pl.ds(pl.multiple_of(block * tall, tall), tall)
            lane = lax.broadcasted_iota(jnp.int32, (tall, narrow), 1)
            head = docs_ref[at, :narrow]
            for nested in range(few):
                cut = jnp.where(lane < uppers[nested], head, jnp.zeros_like(head))
                keep(nested, at, contract(cut, rows_ref[cols_q, :narrow], 1, 1))
            for nested in range(few, WIDTHS):
                cols = slice(lowers[nested], uppers[nested])
                more = contract(docs_ref[at, cols], rows_ref[cols_q, cols], 1, 1)
                keep(nested, at, logits[nested - 1, at, cols_q] + more)
            return carry

        lax.fori_loop(0, count // tall, score_block, 0)

    def soften(part):
        cols_q = turn_cols(part)
        tops = [jnp.max(best[nested], axis=0, keepdims=True) for nested in range(WIDTHS)]
        mass[...] = jnp.zeros_like(mass)
        size = 128

        def mass_block(block, carry):
            at = pl.ds(pl.multiple_of(block * size, size), size)
            for nested in range(WIDTHS):
                piece = logits[nested, at, cols_q] - tops[nested]
                piece = jnp.exp2(piece * (scales[nested] * LOG2_E))
                logits[nested, at, cols_q] = piece
                mass[nested] += jnp.sum(piece.reshape(size // 8, 8, turn), axis=0)
            return carry

        lax.fori_loop(0, count // size, mass_block, 0)
        for nested in range(WIDTHS):
            top = tops[nested] * scales[nested]
            value = top + jnp.log(jnp.sum(mass[nested], axis=0, keepdims=True))
            if nested < 8:
                peaks[part, nested : nested + 1, :turn] = top
                lse[part, nested : nested + 1, :turn] = value
            else:
                for line in range(turn // 128):
                    cols = slice(line * 128, (line + 1) * 128)
                    peaks[part, line : line + 1, turn:] = top[:, cols]
                    lse[part, line : line + 1, turn:] = value[:, cols]

    def share(part):
        return [
            send(lse.at[part], parts.at[part, (chips - step) % chips * 2 + pair - 1], device)
            for step, pair, device in row_peers()
        ]

    def factors(part, copies):
        for copy in copies:
            copy.wait_recv()
        pieces = [lse[part]] + [parts[part, number] for number in range(len(copies))]
        peak = functools.reduce(jnp.maximum, pieces)
        total = peak + jnp.log(sum(jnp.exp(piece - peak) for piece in pieces))
        ratio = jnp.exp(peaks[part] - total)
        rows = [ratio[nested : nested + 1, :turn] * scales[nested] for nested in range(8)]
        tail = [ratio[line : line + 1, turn:] for line in range(turn // 128)]
        return rows + [jnp.concatenate(tail, axis=1) * scales[8]]

    def band(part, factor):
        cols_q = turn_cols(part)

        def band_block(block, carry):
            at = pl.ds(pl.multiple_of(block * own, own), own)
            ids = first_id(block, own) + lax.broadcasted_iota(jnp.int32, (own, turn), 0)
            hit = ids == partner[:, cols_q]
            running = jnp.zeros((own, turn), jnp.float32)
            gone = 0.0
            for nested in reversed(range(WIDTHS)):
                running = running + logits[nested, at, cols_q] * factor[nested]
                gone += scales[nested]
                value = running - jnp.where(hit, gone, 0.0)
                bands[at, turn_cols(part, nested)] = value.astype(jnp.bfloat16)
            return carry

        lax.fori_loop(0, count // own, band_block, 0)

    def bounds(nested):
        return slice(0, narrow) if nested < few else slice(lowers[nested], uppers[nested])

    def product(tall_rows, get, out_ref, at):
        lane = lax.broadcasted_iota(jnp.int32, (tall_rows, narrow), 1)
        head = None
        for nested in range(WIDTHS):
            part = get(nested, bounds(nested))
            if nested < few:
                head = part if head is None else jnp.where(lane < lowers[nested], head, part)
                part = head
            if nested >= few - 1:
                out_ref[at, bounds(nested)] = part

    across = {}

    def d_rows(step, pair, other, lo=0, size=own):
        start = place_of_doc(step, pair, other) * own + lo
        return pl.ds(pl.multiple_of(start, half), size)

    def documents_for(step):
        piece = 4 * own
        chip = lax.rem(lax.axis_index("x") + step, chips)
        at = pl.ds(pl.multiple_of(chip * piece, piece), piece)
        product(
            piece,
            lambda nested, cols: contract(
                bands[at, nested * width : (nested + 1) * width], rows_ref[:, cols], 1, 0
            ),
            pd_ref,
            at,
        )
        for pair in (1, 0):
            theirs = pd_ref.at[d_rows(step, pair, 1), :]
            across[step, pair] = send(theirs, sib.at[step * 2 + pair], sibling)

    def queries_at(chip):
        piece = 2 * own
        product(
            piece,
            lambda nested, cols: contract(
                bands[:, nested * width + chip * piece : nested * width + (chip + 1) * piece],
                docs_ref[:, cols],
                0,
                0,
            ),
            pq_ref,
            slice(chip * piece, (chip + 1) * piece),
        )

    def q_part(step, pair, lo=0, size=own):
        start = place_of_row(step, pair) * own + lo
        return pq_ref[pl.ds(pl.multiple_of(start, half), size), :]

    def d_part(step, pair, lo=0, size=own):
        return pd_ref[d_rows(step, pair, 0, lo, size), :] + sib[step * 2 + pair, pl.ds(lo, size), :]

    lanes = ((q_part, *neighbours("y")), (d_part, *neighbours("x")))
    far = {}
    near = {}

    def send_far(which, pair):
        part, up, down, _ = lanes[which]
        far_s[which, pair] = part(2, pair).astype(jnp.bfloat16)
        for way, device in ((0, up), (1, down)):
            piece = pl.ds(way * half, half)
            far[which, pair, way] = send(
                far_s.at[which, pair, piece], far_r.at[which, pair, piece], device
            )

    def send_near(which, pair):
        part, up, down, _ = lanes[which]
        for way, device, step in ((0, up, 1), (1, down, 3)):
            if which == 1:
                across[step, pair].wait_recv()
            far[which, pair, way].wait_recv()
            lo = way * half
            more = half - lo
            near_s[which, pair, way, pl.ds(lo, half), :] = (
                part(step, pair, lo, half)
                + far_r[which, pair, pl.ds(lo, half), :].astype(jnp.float32)
            ).astype(jnp.bfloat16)
            near_s[which, pair, way, pl.ds(more, half), :] = part(step, pair, more, half).astype(
                jnp.bfloat16
            )
            near[which, pair, way] = send(
                near_s.at[which, pair, way], near_r.at[which, pair, way], device
            )

    def arrived(which, pair):
        part = lanes[which][0]
        if which == 1:
            across[0, pair].wait_recv()
        near[which, pair, 0].wait_recv()
        near[which, pair, 1].wait_recv()
        return (
            part(0, pair)
            + near_r[which, pair, 0].astype(jnp.float32)
            + near_r[which, pair, 1].astype(jnp.float32)
        )

    shared = []
    for part in range(2):
        score(part)
        soften(part)
        shared.append(share(part))
    band(0, factors(0, shared[0]))
    queries_at(0)
    queries_at(1)
    band(1, factors(1, shared[1]))
    documents_for(2)
    queries_at(2)
    queries_at(3)
    send_far(0, 1)
    send_far(0, 0)
    for pair in (1, 0):
        across[2, pair].wait_recv()
        send_far(1, pair)
    documents_for(1)
    documents_for(3)
    for pair in (1, 0):
        send_near(0, pair)
        send_near(1, pair)
    documents_for(0)
    last = []
    for which in range(2):
        pair_s[which] = arrived(which, 1).astype(jnp.bfloat16)
        last.append(send(pair_s.at[which], pair_r.at[which], lanes[which][3]))
    outs = (gq_ref, gd_ref)
    for which in range(2):
        outs[which][...] = arrived(which, 0)
    for which in range(2):
        last[which].wait_recv()
        outs[which][...] = outs[which][...] + pair_r[which].astype(jnp.float32)
    send.finish()


def on_device(queries, documents, partner):
    own, dim = queries.shape
    width, count = 8 * own, 16 * own
    piece = jax.ShapeDtypeStruct((own, dim), jnp.float32)
    wire = jnp.bfloat16
    copies = 7 + 26 + 14 + 30
    return pl.pallas_call(
        step_kernel,
        out_shape=(piece, piece),
        in_specs=[VMEM] * 3,
        out_specs=(VMEM, VMEM),
        scratch_shapes=[
            pltpu.VMEM((width, dim), wire),
            pltpu.VMEM((count, dim), wire),
            pltpu.VMEM((WIDTHS, count, width), jnp.float32),
            pltpu.VMEM((count, WIDTHS * width), wire),
            pltpu.VMEM((WIDTHS, 8, width // 2), jnp.float32),
            pltpu.VMEM((WIDTHS, 8, width // 2), jnp.float32),
            pltpu.VMEM((2, 8, width // 2 + 128), jnp.float32),
            pltpu.VMEM((2, 8, width // 2 + 128), jnp.float32),
            pltpu.VMEM((2, 7, 8, width // 2 + 128), jnp.float32),
            pltpu.VMEM((8, 8, 2 * own), jnp.int32),
            pltpu.VMEM((width, dim), jnp.float32),
            pltpu.VMEM((count, dim), jnp.float32),
            pltpu.VMEM((8, own, dim), jnp.float32),
            pltpu.VMEM((2, 2, own, dim), wire),
            pltpu.VMEM((2, 2, 2, own, dim), wire),
            pltpu.VMEM((2, 2, own, dim), wire),
            pltpu.VMEM((2, 2, 2, own, dim), wire),
            pltpu.VMEM((2, own, dim), wire),
            pltpu.VMEM((2, own, dim), wire),
            pltpu.SemaphoreType.DMA((copies,)),
            pltpu.SemaphoreType.DMA((copies,)),
        ],
        compiler_params=pltpu.CompilerParams(
            collective_id=0, has_side_effects=True, vmem_limit_bytes=67043328
        ),
        name="step",
    )(queries, documents, jnp.tile(partner[None, :], (8, 2)))


def solution(mesh):
    finer = Mesh(mesh.devices.reshape(4, 2, 4, 2, mesh.shape["rep"]), AXES)
    placed = (P(AXES, None), P(AXES, None), P(AXES))
    return jax.shard_map(
        on_device,
        mesh=finer,
        in_specs=placed,
        out_specs=(P(AXES, None), P(AXES, None)),
        check_vma=False,
    )
```

```python
import functools
import jax
import jax.numpy as jnp
from jax import lax
from jax.experimental import pallas as pl
from jax.experimental.pallas import tpu as pltpu
from jax.sharding import Mesh
from jax.sharding import PartitionSpec as P

WIDTHS = 9
LOG2_E = 1.4426950408889634
logit_gain = 3.0

AXES = ("y", "zl", "x", "core", "zh")
MESH = pl.DeviceIdType.MESH
VMEM = pl.BlockSpec(memory_space=pltpu.VMEM)


def width_list(feature_dim):
    return [feature_dim >> WIDTHS - 1 - nested for nested in range(WIDTHS)]


def split_at(dim):
    return dim * 9 // 16


def contract(first_op, second_op, first_dim, second_dim):
    return lax.dot_general(
        first_op,
        second_op,
        (((first_dim,), (second_dim,)), ((), ())),
        preferred_element_type=jnp.float32,
    )


def neighbours(axis):
    size = lax.axis_size(axis)
    me = lax.axis_index(axis)
    up = {axis: lax.rem(me + 1, size)}
    down = {axis: lax.rem(me + size - 1, size)}
    pair = {"zl": 1 - lax.axis_index("zl")}
    if axis == "x":
        pair["zh"] = 1 - lax.axis_index("zh")
    return up, down, pair


def row_peers():
    chips = lax.axis_size("y")
    y = lax.axis_index("y")
    zl = lax.axis_index("zl")
    return [
        (step, pair, {"y": lax.rem(y + step, chips), "zl": lax.rem(zl + pair, 2)})
        for step in range(chips)
        for pair in range(2)
        if step or pair
    ]


def place_of_row(step, pair):
    y = lax.rem(lax.axis_index("y") + step, lax.axis_size("y"))
    return y * 2 + lax.rem(lax.axis_index("zl") + pair, 2)


def place_of_doc(step, pair, other):
    x = lax.rem(lax.axis_index("x") + step, lax.axis_size("x"))
    zh = lax.rem(lax.axis_index("zh") + pair, 2)
    return (x * 2 + zh) * 2 + lax.rem(lax.axis_index("core") + other, 2)


def first_id(place, own):
    x, there, core = place // 4, lax.rem(place // 2, 2), lax.rem(place, 2)
    zl = lax.rem(lax.axis_index("zl") + lax.axis_index("zh") + there, 2)
    chip = (lax.axis_index("y") * 2 + zl) * lax.axis_size("x") + x
    return ((chip * 2 + core) * 2 + there) * own


def meet(devices):
    barrier = pltpu.get_barrier_semaphore()
    for device in devices:
        pl.semaphore_signal(barrier, inc=1, device_id=device, device_id_type=MESH)
    pl.semaphore_wait(barrier, len(devices))


class Sender:
    def __init__(self, sent, landed):
        self.sent, self.landed, self.started = sent, landed, []

    def __call__(self, src, dst, device):
        number = len(self.started)
        copy = pltpu.make_async_remote_copy(
            src_ref=src,
            dst_ref=dst,
            send_sem=self.sent.at[number],
            recv_sem=self.landed.at[number],
            device_id=device,
            device_id_type=MESH,
        )
        copy.start()
        self.started.append(copy)
        return copy

    def finish(self):
        for copy in self.started:
            copy.wait_send()


def gather(send, rows_ref, docs_ref, own):
    half = own // 2
    sibling = {"core": 1 - lax.axis_index("core")}
    dim = docs_ref.shape[1]
    early, late, every = slice(0, split_at(dim)), slice(split_at(dim), dim), slice(0, dim)

    def q_slot(step, pair, cols, lo=0, size=own):
        start = place_of_row(step, pair) * own + lo
        return rows_ref.at[pl.ds(pl.multiple_of(start, half), size), cols]

    def d_slot(step, pair, cols, lo=0, size=own):
        start = place_of_doc(step, pair, 0) * own + lo
        return docs_ref.at[pl.ds(pl.multiple_of(start, half), size), cols]

    lanes = ((d_slot, *neighbours("x")), (q_slot, *neighbours("y")))
    across = []

    def cross(which, step, pair, cols):
        if which == 0:
            piece = d_slot(step, pair, cols)
            across.append(send(piece, piece, sibling))

    def onward(piece, device):
        return send(piece, piece, device)

    own_early, own_late, up_late, down_late, up_early, down_early = ([] for _ in range(6))
    for slot, up, down, pair in lanes:
        own_early.append(onward(slot(0, 0, early), pair))
        up_late.append(onward(slot(0, 0, late), up))
        down_late.append(onward(slot(0, 0, late), down))
        up_early.append(onward(slot(0, 0, early), up))
        down_early.append(onward(slot(0, 0, early), down))
        own_late.append(onward(slot(0, 0, late), pair))
    cross(0, 0, 0, every)

    def relay(which, step_pair, cols, copies):
        slot, up, down, _ = lanes[which]
        from_down, from_up = copies
        from_down.wait_recv()
        first = onward(slot(3, step_pair, cols, 0, half), up)
        from_up.wait_recv()
        return first, onward(slot(1, step_pair, cols, half, half), down)

    far_late, back_late, beside, far_early, far_pair, last_late = ([] for _ in range(6))
    for which, (slot, up, down, pair) in enumerate(lanes):
        far_late.append(relay(which, 0, late, (up_late[which], down_late[which])))
        back_late.append([onward(slot(step, 0, late), pair) for step in (3, 1)])
    for which, (slot, up, down, pair) in enumerate(lanes):
        own_early[which].wait_recv()
        beside.append([onward(slot(0, 1, early), device) for device in (up, down)])
        cross(which, 0, 1, early)
    for which in range(2):
        far_early.append(relay(which, 0, early, (up_early[which], down_early[which])))
        cross(which, 3, 0, every)
        cross(which, 1, 0, every)
    for which, (slot, up, down, pair) in enumerate(lanes):
        for copy in far_late[which]:
            copy.wait_recv()
        last_late.append(onward(slot(2, 0, late), pair))
        cross(which, 2, 0, late)
        own_late[which].wait_recv()
        cross(which, 0, 1, late)
    for which in range(2):
        far_pair.append(relay(which, 1, early, beside[which]))
        for copy in back_late[which]:
            copy.wait_recv()
        cross(which, 3, 1, every)
        cross(which, 1, 1, every)
    for which in range(2):
        for copy in far_early[which]:
            copy.wait_recv()
        cross(which, 2, 0, early)
    for which in range(2):
        last_late[which].wait_recv()
        cross(which, 2, 1, late)
        for copy in far_pair[which]:
            copy.wait_recv()
        cross(which, 2, 1, early)
    for copy in across:
        copy.wait_recv()


def step_kernel(
    q_ref,
    d_ref,
    p_ref,
    gq_ref,
    gd_ref,
    rows_ref,
    docs_ref,
    logits,
    bands,
    best,
    mass,
    peaks,
    lse,
    parts,
    marks,
    pq_ref,
    pd_ref,
    sib,
    far_s,
    near_s,
    far_r,
    near_r,
    pair_s,
    pair_r,
    cross_s,
    cross_r,
    inside,
    sent,
    landed,
):
    count, dim = docs_ref.shape
    width = rows_ref.shape[0]
    own = q_ref.shape[0]
    half = own // 2
    uppers = width_list(dim)
    lowers = [0] + uppers[:-1]
    scales = [logit_gain * upper ** (-0.5) for upper in uppers]
    narrow = 256
    few = uppers.index(narrow) + 1
    chips = lax.axis_size("y")
    sibling = {"core": 1 - lax.axis_index("core")}
    send = Sender(sent, landed)

    q_place = pl.ds(pl.multiple_of(place_of_row(0, 0) * own, own), own)
    d_place = pl.ds(pl.multiple_of(place_of_doc(0, 0, 0) * own, own), own)
    taken = [
        pltpu.make_async_copy(d_ref, docs_ref.at[d_place, :], inside.at[0]),
        pltpu.make_async_copy(q_ref, rows_ref.at[q_place, :], inside.at[1]),
    ]
    for copy in taken:
        copy.start()
    meet([*neighbours("y"), *neighbours("x"), sibling])
    for copy in taken:
        copy.wait()
    marks[place_of_row(0, 0)] = p_ref[...]
    lse[...] = jnp.zeros_like(lse)
    peaks[...] = jnp.zeros_like(peaks)
    gather(send, rows_ref, docs_ref, own)
    marked = [send(p_ref, marks.at[place_of_row(0, 0)], device) for _, _, device in row_peers()]

    turn = width // 2
    tall = count // 2

    def turn_cols(part, nested=0):
        start = nested * width + part * turn
        return slice(start, start + turn)

    def score(part):
        cols_q = turn_cols(part)
        best[...] = jnp.full(best.shape, -jnp.inf, jnp.float32)

        def keep(nested, at, value):
            logits[nested, at, cols_q] = value
            top = jnp.max(value.reshape(tall // 8, 8, turn), axis=0)
            best[nested] = jnp.maximum(best[nested], top)

        def score_block(block, carry):
            at = pl.ds(pl.multiple_of(block * tall, tall), tall)
            lane = lax.broadcasted_iota(jnp.int32, (tall, narrow), 1)
            head = docs_ref[at, :narrow]
            for nested in range(few):
                cut = jnp.where(lane < uppers[nested], head, jnp.zeros_like(head))
                keep(nested, at, contract(cut, rows_ref[cols_q, :narrow], 1, 1))
            for nested in range(few, WIDTHS):
                cols = slice(lowers[nested], uppers[nested])
                more = contract(docs_ref[at, cols], rows_ref[cols_q, cols], 1, 1)
                keep(nested, at, logits[nested - 1, at, cols_q] + more)
            return carry

        lax.fori_loop(0, count // tall, score_block, 0)

    def soften(part):
        cols_q = turn_cols(part)
        tops = [jnp.max(best[nested], axis=0, keepdims=True) for nested in range(WIDTHS)]
        mass[...] = jnp.zeros_like(mass)
        size = 128

        def mass_block(block, carry):
            at = pl.ds(pl.multiple_of(block * size, size), size)
            for nested in range(WIDTHS):
                piece = logits[nested, at, cols_q] - tops[nested]
                piece = jnp.exp2(piece * (scales[nested] * LOG2_E))
                logits[nested, at, cols_q] = piece
                mass[nested] += jnp.sum(piece.reshape(size // 8, 8, turn), axis=0)
            return carry

        lax.fori_loop(0, count // size, mass_block, 0)
        for nested in range(WIDTHS):
            top = tops[nested] * scales[nested]
            value = top + jnp.log(jnp.sum(mass[nested], axis=0, keepdims=True))
            if nested < 8:
                peaks[part, nested : nested + 1, :turn] = top
                lse[part, nested : nested + 1, :turn] = value
            else:
                for line in range(turn // 128):
                    cols = slice(line * 128, (line + 1) * 128)
                    peaks[part, line : line + 1, turn:] = top[:, cols]
                    lse[part, line : line + 1, turn:] = value[:, cols]

    def share(part):
        return [
            send(lse.at[part], parts.at[part, (chips - step) % chips * 2 + pair - 1], device)
            for step, pair, device in row_peers()
        ]

    def factors(part, copies):
        for copy in copies:
            copy.wait_recv()
        pieces = [lse[part]] + [parts[part, number] for number in range(len(copies))]
        peak = functools.reduce(jnp.maximum, pieces)
        total = peak + jnp.log(sum(jnp.exp(piece - peak) for piece in pieces))
        ratio = jnp.exp(peaks[part] - total)
        rows = [ratio[nested : nested + 1, :turn] * scales[nested] for nested in range(8)]
        tail = [ratio[line : line + 1, turn:] for line in range(turn // 128)]
        return rows + [jnp.concatenate(tail, axis=1) * scales[8]]

    def band(part, factor, partner):
        cols_q = turn_cols(part)

        def band_block(block, carry):
            at = pl.ds(pl.multiple_of(block * own, own), own)
            ids = first_id(block, own) + lax.broadcasted_iota(jnp.int32, (own, turn), 0)
            hit = ids == partner[:, cols_q]
            running = jnp.zeros((own, turn), jnp.float32)
            gone = 0.0
            for nested in reversed(range(WIDTHS)):
                running = running + logits[nested, at, cols_q] * factor[nested]
                gone += scales[nested]
                value = running - jnp.where(hit, gone, 0.0)
                bands[at, turn_cols(part, nested)] = value.astype(jnp.bfloat16)
            return carry

        lax.fori_loop(0, count // own, band_block, 0)

    def bounds(nested):
        return slice(0, narrow) if nested < few else slice(lowers[nested], uppers[nested])

    def product(tall_rows, get, out_ref, at):
        lane = lax.broadcasted_iota(jnp.int32, (tall_rows, narrow), 1)
        head = None
        for nested in range(WIDTHS):
            part = get(nested, bounds(nested))
            if nested < few:
                head = part if head is None else jnp.where(lane < lowers[nested], head, part)
                part = head
            if nested >= few - 1:
                out_ref[at, bounds(nested)] = part

    across = {}

    def d_rows(step, pair, other, lo=0, size=own):
        start = place_of_doc(step, pair, other) * own + lo
        return pl.ds(pl.multiple_of(start, half), size)

    def documents_for(step):
        piece = 4 * own
        chip = lax.rem(lax.axis_index("x") + step, chips)
        at = pl.ds(pl.multiple_of(chip * piece, piece), piece)
        product(
            piece,
            lambda nested, cols: contract(
                bands[at, nested * width : (nested + 1) * width], rows_ref[:, cols], 1, 0
            ),
            pd_ref,
            at,
        )
        for pair in (1, 0):
            theirs = pd_ref.at[d_rows(step, pair, 1), :]
            across[step, pair] = send(theirs, sib.at[step * 2 + pair], sibling)

    def queries_at(chip):
        piece = 2 * own
        product(
            piece,
            lambda nested, cols: contract(
                bands[:, nested * width + chip * piece : nested * width + (chip + 1) * piece],
                docs_ref[:, cols],
                0,
                0,
            ),
            pq_ref,
            slice(chip * piece, (chip + 1) * piece),
        )

    def q_part(step, pair, lo, size, cols):
        start = place_of_row(step, pair) * own + lo
        return pq_ref[pl.ds(pl.multiple_of(start, half), size), cols]

    def d_part(step, pair, lo, size, cols):
        arrive(across[step, pair])
        mine = pd_ref[d_rows(step, pair, 0, lo, size), cols]
        return mine + sib[step * 2 + pair, pl.ds(lo, size), cols]

    waited = []

    def arrive(copy):
        if not any(copy is seen for seen in waited):
            copy.wait_recv()
            waited.append(copy)

    lanes = ((q_part, *neighbours("y")), (d_part, *neighbours("x")))
    edge = split_at(dim)
    early, late = slice(0, edge), slice(edge, dim)
    crossed, far, near = {}, {}, {}

    def cross(which, step):
        part, _, _, pair = lanes[which]
        cross_s[which, step] = part(step, 1, 0, own, late).astype(jnp.bfloat16)
        crossed[which, step] = send(cross_s.at[which, step], cross_r.at[which, step], pair)

    def term(which, pair, cols, step, lo, size):
        value = lanes[which][0](step, pair, lo, size, cols)
        if cols is late:
            arrive(crossed[which, step])
            value = value + cross_r[which, step, pl.ds(lo, size), :].astype(jnp.float32)
        return value

    def send_far(which, pair, cols):
        _, up, down, _ = lanes[which]
        far_s[which, pair, :, cols] = term(which, pair, cols, 2, 0, own).astype(jnp.bfloat16)
        for way, device in ((0, up), (1, down)):
            piece = pl.ds(way * half, half)
            far[which, pair, cols.start, way] = send(
                far_s.at[which, pair, piece, cols], far_r.at[which, pair, piece, cols], device
            )

    def send_near(which, pair, cols):
        _, up, down, _ = lanes[which]
        for way, device, step in ((0, up, 1), (1, down, 3)):
            lo = way * half
            more = half - lo
            near_s[which, pair, way, pl.ds(more, half), cols] = term(
                which, pair, cols, step, more, half
            ).astype(jnp.bfloat16)
            mine = term(which, pair, cols, step, lo, half)
            arrive(far[which, pair, cols.start, way])
            near_s[which, pair, way, pl.ds(lo, half), cols] = (
                mine + far_r[which, pair, pl.ds(lo, half), cols].astype(jnp.float32)
            ).astype(jnp.bfloat16)
            near[which, pair, cols.start, way] = send(
                near_s.at[which, pair, way, :, cols], near_r.at[which, pair, way, :, cols], device
            )

    def summed(which, pair, cols):
        value = term(which, pair, cols, 0, 0, own)
        for way in range(2):
            arrive(near[which, pair, cols.start, way])
            value = value + near_r[which, pair, way, :, cols].astype(jnp.float32)
        return value

    shared = []
    for part in range(2):
        score(part)
        soften(part)
        shared.append(share(part))
    for copy in marked:
        copy.wait_recv()
    side = lax.broadcasted_iota(jnp.int32, (1, 2 * own), 1)
    partner = jnp.concatenate(
        [
            jnp.where(side < own, marks[2 * step, 0:1, :], marks[2 * step + 1, 0:1, :])
            for step in range(chips)
        ],
        axis=1,
    )
    band(0, factors(0, shared[0]), partner)
    queries_at(0)
    queries_at(1)
    band(1, factors(1, shared[1]), partner)
    documents_for(2)
    queries_at(2)
    queries_at(3)
    for which in range(2):
        cross(which, 2)
        send_far(which, 1, early)
        send_far(which, 0, early)
    for step in (1, 3, 0):
        cross(0, step)
    documents_for(1)
    documents_for(3)
    for which in range(2):
        send_far(which, 0, late)
    cross(1, 1)
    cross(1, 3)
    for which in range(2):
        send_near(which, 1, early)
    documents_for(0)
    for which in range(2):
        send_near(which, 0, early)
    cross(1, 0)
    for which in range(2):
        send_near(which, 0, late)
    outs = (gq_ref, gd_ref)
    last = []
    for which in range(2):
        pair_s[which] = summed(which, 1, early).astype(jnp.bfloat16)
        last.append(send(pair_s.at[which], pair_r.at[which], lanes[which][3]))
    for which in range(2):
        outs[which][:, early] = summed(which, 0, early)
    for which in range(2):
        outs[which][:, late] = summed(which, 0, late)
    for which in range(2):
        last[which].wait_recv()
        outs[which][:, early] = outs[which][:, early] + pair_r[which].astype(jnp.float32)
    send.finish()


def on_device(queries, documents, partner):
    own, dim = queries.shape
    width, count = 8 * own, 16 * own
    piece = jax.ShapeDtypeStruct((own, dim), jnp.float32)
    wire = jnp.bfloat16
    edge = split_at(dim)
    copies = 120
    return pl.pallas_call(
        step_kernel,
        out_shape=(piece, piece),
        in_specs=[pl.BlockSpec(memory_space=pl.ANY)] * 2 + [VMEM],
        out_specs=(VMEM, VMEM),
        scratch_shapes=[
            pltpu.VMEM((width, dim), wire),
            pltpu.VMEM((count, dim), wire),
            pltpu.VMEM((WIDTHS, count, width), jnp.float32),
            pltpu.VMEM((count, WIDTHS * width), wire),
            pltpu.VMEM((WIDTHS, 8, width // 2), jnp.float32),
            pltpu.VMEM((WIDTHS, 8, width // 2), jnp.float32),
            pltpu.VMEM((2, 8, width // 2 + 128), jnp.float32),
            pltpu.VMEM((2, 8, width // 2 + 128), jnp.float32),
            pltpu.VMEM((2, 7, 8, width // 2 + 128), jnp.float32),
            pltpu.VMEM((8, 8, 2 * own), jnp.int32),
            pltpu.VMEM((width, dim), jnp.float32),
            pltpu.VMEM((count, dim), jnp.float32),
            pltpu.VMEM((8, own, dim), jnp.float32),
            pltpu.VMEM((2, 2, own, dim), wire),
            pltpu.VMEM((2, 2, 2, own, dim), wire),
            pltpu.VMEM((2, 2, own, dim), wire),
            pltpu.VMEM((2, 2, 2, own, dim), wire),
            pltpu.VMEM((2, own, edge), wire),
            pltpu.VMEM((2, own, edge), wire),
            pltpu.VMEM((2, 4, own, dim - edge), wire),
            pltpu.VMEM((2, 4, own, dim - edge), wire),
            pltpu.SemaphoreType.DMA((2,)),
            pltpu.SemaphoreType.DMA((copies,)),
            pltpu.SemaphoreType.DMA((copies,)),
        ],
        compiler_params=pltpu.CompilerParams(
            collective_id=0, has_side_effects=True, vmem_limit_bytes=67043328
        ),
        name="step",
    )(queries, documents, jnp.tile(partner[None, :], (8, 2)))


def solution(mesh):
    finer = Mesh(mesh.devices.reshape(4, 2, 4, 2, mesh.shape["rep"]), AXES)
    placed = (P(AXES, None), P(AXES, None), P(AXES))
    return jax.shard_map(
        on_device,
        mesh=finer,
        in_specs=placed,
        out_specs=(P(AXES, None), P(AXES, None)),
        check_vma=False,
    )
```

```python
import functools
import jax
import jax.numpy as jnp
from jax import lax
from jax.experimental import pallas as pl
from jax.experimental.pallas import tpu as pltpu
from jax.sharding import Mesh
from jax.sharding import PartitionSpec as P

WIDTHS = 9
LOG2_E = 1.4426950408889634
logit_gain = 3.0

AXES = ("y", "zl", "x", "core", "zh")
MESH = pl.DeviceIdType.MESH
VMEM = pl.BlockSpec(memory_space=pltpu.VMEM)


def width_list(feature_dim):
    return [feature_dim >> WIDTHS - 1 - nested for nested in range(WIDTHS)]


def split_at(dim):
    return dim * 9 // 16


def contract(first_op, second_op, first_dim, second_dim):
    return lax.dot_general(
        first_op,
        second_op,
        (((first_dim,), (second_dim,)), ((), ())),
        preferred_element_type=jnp.float32,
    )


def neighbours(axis):
    size = lax.axis_size(axis)
    me = lax.axis_index(axis)
    up = {axis: lax.rem(me + 1, size)}
    down = {axis: lax.rem(me + size - 1, size)}
    pair = {"zl": 1 - lax.axis_index("zl")}
    if axis == "x":
        pair["zh"] = 1 - lax.axis_index("zh")
    return up, down, pair


def row_peers():
    chips = lax.axis_size("y")
    y = lax.axis_index("y")
    zl = lax.axis_index("zl")
    return [
        (step, pair, {"y": lax.rem(y + step, chips), "zl": lax.rem(zl + pair, 2)})
        for step in range(chips)
        for pair in range(2)
        if step or pair
    ]


def place_of_row(step, pair):
    y = lax.rem(lax.axis_index("y") + step, lax.axis_size("y"))
    return y * 2 + lax.rem(lax.axis_index("zl") + pair, 2)


def place_of_doc(step, pair, other):
    x = lax.rem(lax.axis_index("x") + step, lax.axis_size("x"))
    zh = lax.rem(lax.axis_index("zh") + pair, 2)
    return (x * 2 + zh) * 2 + lax.rem(lax.axis_index("core") + other, 2)


def first_id(place, own):
    x, there, core = place // 4, lax.rem(place // 2, 2), lax.rem(place, 2)
    zl = lax.rem(lax.axis_index("zl") + lax.axis_index("zh") + there, 2)
    chip = (lax.axis_index("y") * 2 + zl) * lax.axis_size("x") + x
    return ((chip * 2 + core) * 2 + there) * own


def meet(devices):
    barrier = pltpu.get_barrier_semaphore()
    for device in devices:
        pl.semaphore_signal(barrier, inc=1, device_id=device, device_id_type=MESH)
    pl.semaphore_wait(barrier, len(devices))


class Sender:
    def __init__(self, sent, landed):
        self.sent, self.landed, self.started = sent, landed, []

    def __call__(self, src, dst, device):
        number = len(self.started)
        copy = pltpu.make_async_remote_copy(
            src_ref=src,
            dst_ref=dst,
            send_sem=self.sent.at[number],
            recv_sem=self.landed.at[number],
            device_id=device,
            device_id_type=MESH,
        )
        copy.start()
        self.started.append(copy)
        return copy

    def finish(self):
        for copy in self.started:
            copy.wait_send()


def gather(send, rows_ref, docs_ref, own):
    half = own // 2
    sibling = {"core": 1 - lax.axis_index("core")}
    dim = docs_ref.shape[1]
    early, late, every = slice(0, split_at(dim)), slice(split_at(dim), dim), slice(0, dim)

    def q_slot(step, pair, cols, lo=0, size=own):
        start = place_of_row(step, pair) * own + lo
        return rows_ref.at[pl.ds(pl.multiple_of(start, half), size), cols]

    def d_slot(step, pair, cols, lo=0, size=own):
        start = place_of_doc(step, pair, 0) * own + lo
        return docs_ref.at[pl.ds(pl.multiple_of(start, half), size), cols]

    lanes = ((d_slot, *neighbours("x")), (q_slot, *neighbours("y")))
    across = []

    def cross(which, step, pair, cols):
        if which == 0:
            piece = d_slot(step, pair, cols)
            across.append(send(piece, piece, sibling))

    def onward(piece, device):
        return send(piece, piece, device)

    own_early, own_late, up_late, down_late, up_early, down_early = ([] for _ in range(6))
    for slot, up, down, pair in lanes:
        own_early.append(onward(slot(0, 0, early), pair))
        up_late.append(onward(slot(0, 0, late), up))
        down_late.append(onward(slot(0, 0, late), down))
        up_early.append(onward(slot(0, 0, early), up))
        down_early.append(onward(slot(0, 0, early), down))
        own_late.append(onward(slot(0, 0, late), pair))
    cross(0, 0, 0, every)

    def relay(which, step_pair, cols, copies):
        slot, up, down, _ = lanes[which]
        from_down, from_up = copies
        from_down.wait_recv()
        first = onward(slot(3, step_pair, cols, 0, half), up)
        from_up.wait_recv()
        return first, onward(slot(1, step_pair, cols, half, half), down)

    far_late, back_late, beside, far_early, far_pair, last_late = ([] for _ in range(6))
    for which, (slot, up, down, pair) in enumerate(lanes):
        far_late.append(relay(which, 0, late, (up_late[which], down_late[which])))
        back_late.append([onward(slot(step, 0, late), pair) for step in (3, 1)])
    for which, (slot, up, down, pair) in enumerate(lanes):
        own_early[which].wait_recv()
        beside.append([onward(slot(0, 1, early), device) for device in (up, down)])
        cross(which, 0, 1, early)
    for which in range(2):
        far_early.append(relay(which, 0, early, (up_early[which], down_early[which])))
        cross(which, 3, 0, every)
        cross(which, 1, 0, every)
    for which, (slot, up, down, pair) in enumerate(lanes):
        for copy in far_late[which]:
            copy.wait_recv()
        last_late.append(onward(slot(2, 0, late), pair))
        cross(which, 2, 0, late)
        own_late[which].wait_recv()
        cross(which, 0, 1, late)
    for which in range(2):
        far_pair.append(relay(which, 1, early, beside[which]))
        for copy in back_late[which]:
            copy.wait_recv()
        cross(which, 3, 1, every)
        cross(which, 1, 1, every)
    for which in range(2):
        for copy in far_early[which]:
            copy.wait_recv()
        cross(which, 2, 0, early)
    for which in range(2):
        last_late[which].wait_recv()
        cross(which, 2, 1, late)
        for copy in far_pair[which]:
            copy.wait_recv()
        cross(which, 2, 1, early)
    for copy in across:
        copy.wait_recv()


def step_kernel(
    q_ref,
    d_ref,
    p_ref,
    gq_ref,
    gd_ref,
    rows_ref,
    docs_ref,
    logits,
    bands,
    best,
    mass,
    peaks,
    lse,
    parts,
    marks,
    pq_ref,
    pd_ref,
    sib,
    far_s,
    near_s,
    far_r,
    near_r,
    pair_s,
    pair_r,
    cross_s,
    cross_r,
    inside,
    sent,
    landed,
):
    count, dim = docs_ref.shape
    width = rows_ref.shape[0]
    own = q_ref.shape[0]
    half = own // 2
    uppers = width_list(dim)
    lowers = [0] + uppers[:-1]
    scales = [logit_gain * upper ** (-0.5) for upper in uppers]
    narrow = 256
    few = uppers.index(narrow) + 1
    chips = lax.axis_size("y")
    sibling = {"core": 1 - lax.axis_index("core")}
    send = Sender(sent, landed)

    q_place = pl.ds(pl.multiple_of(place_of_row(0, 0) * own, own), own)
    d_place = pl.ds(pl.multiple_of(place_of_doc(0, 0, 0) * own, own), own)
    taken = [
        pltpu.make_async_copy(d_ref, docs_ref.at[d_place, :], inside.at[0]),
        pltpu.make_async_copy(q_ref, rows_ref.at[q_place, :], inside.at[1]),
    ]
    for copy in taken:
        copy.start()
    meet([*neighbours("y"), *neighbours("x"), sibling])
    for copy in taken:
        copy.wait()
    marks[place_of_row(0, 0)] = p_ref[...]
    lse[...] = jnp.zeros_like(lse)
    peaks[...] = jnp.zeros_like(peaks)
    gather(send, rows_ref, docs_ref, own)
    marked = [send(p_ref, marks.at[place_of_row(0, 0)], device) for _, _, device in row_peers()]

    turn = width // 2
    tall = count // 2

    def turn_cols(part, nested=0):
        start = nested * width + part * turn
        return slice(start, start + turn)

    def score(part):
        cols_q = turn_cols(part)
        best[...] = jnp.full(best.shape, -jnp.inf, jnp.float32)

        def keep(nested, at, value):
            logits[nested, at, cols_q] = value
            top = jnp.max(value.reshape(tall // 8, 8, turn), axis=0)
            best[nested] = jnp.maximum(best[nested], top)

        def score_block(block, carry):
            at = pl.ds(pl.multiple_of(block * tall, tall), tall)
            lane = lax.broadcasted_iota(jnp.int32, (tall, narrow), 1)
            head = docs_ref[at, :narrow]
            for nested in range(few):
                cut = jnp.where(lane < uppers[nested], head, jnp.zeros_like(head))
                keep(nested, at, contract(cut, rows_ref[cols_q, :narrow], 1, 1))
            for nested in range(few, WIDTHS):
                cols = slice(lowers[nested], uppers[nested])
                more = contract(docs_ref[at, cols], rows_ref[cols_q, cols], 1, 1)
                keep(nested, at, logits[nested - 1, at, cols_q] + more)
            return carry

        lax.fori_loop(0, count // tall, score_block, 0)

    def soften(part):
        cols_q = turn_cols(part)
        tops = [jnp.max(best[nested], axis=0, keepdims=True) for nested in range(WIDTHS)]
        mass[...] = jnp.zeros_like(mass)
        size = 128

        def mass_block(block, carry):
            at = pl.ds(pl.multiple_of(block * size, size), size)
            for nested in range(WIDTHS):
                piece = logits[nested, at, cols_q] - tops[nested]
                piece = jnp.exp2(piece * (scales[nested] * LOG2_E))
                logits[nested, at, cols_q] = piece
                mass[nested] += jnp.sum(piece.reshape(size // 8, 8, turn), axis=0)
            return carry

        lax.fori_loop(0, count // size, mass_block, 0)
        for nested in range(WIDTHS):
            top = tops[nested] * scales[nested]
            value = top + jnp.log(jnp.sum(mass[nested], axis=0, keepdims=True))
            if nested < 8:
                peaks[part, nested : nested + 1, :turn] = top
                lse[part, nested : nested + 1, :turn] = value
            else:
                for line in range(turn // 128):
                    cols = slice(line * 128, (line + 1) * 128)
                    peaks[part, line : line + 1, turn:] = top[:, cols]
                    lse[part, line : line + 1, turn:] = value[:, cols]

    def share(part):
        return [
            send(lse.at[part], parts.at[part, (chips - step) % chips * 2 + pair - 1], device)
            for step, pair, device in row_peers()
        ]

    def factors(part, copies):
        for copy in copies:
            copy.wait_recv()
        pieces = [lse[part]] + [parts[part, number] for number in range(len(copies))]
        peak = functools.reduce(jnp.maximum, pieces)
        total = peak + jnp.log(sum(jnp.exp(piece - peak) for piece in pieces))
        ratio = jnp.exp(peaks[part] - total)
        rows = [ratio[nested : nested + 1, :turn] * scales[nested] for nested in range(8)]
        tail = [ratio[line : line + 1, turn:] for line in range(turn // 128)]
        return rows + [jnp.concatenate(tail, axis=1) * scales[8]]

    def band(part, factor, partner):
        cols_q = turn_cols(part)

        def band_block(block, carry):
            at = pl.ds(pl.multiple_of(block * own, own), own)
            ids = first_id(block, own) + lax.broadcasted_iota(jnp.int32, (own, turn), 0)
            hit = ids == partner[:, cols_q]
            running = jnp.zeros((own, turn), jnp.float32)
            gone = 0.0
            for nested in reversed(range(WIDTHS)):
                running = running + logits[nested, at, cols_q] * factor[nested]
                gone += scales[nested]
                value = running - jnp.where(hit, gone, 0.0)
                bands[at, turn_cols(part, nested)] = value.astype(jnp.bfloat16)
            return carry

        lax.fori_loop(0, count // own, band_block, 0)

    def bounds(nested):
        return slice(0, narrow) if nested < few else slice(lowers[nested], uppers[nested])

    def product(tall_rows, get, out_ref, at):
        lane = lax.broadcasted_iota(jnp.int32, (tall_rows, narrow), 1)
        head = None
        for nested in range(WIDTHS):
            part = get(nested, bounds(nested))
            if nested < few:
                head = part if head is None else jnp.where(lane < lowers[nested], head, part)
                part = head
            if nested >= few - 1:
                out_ref[at, bounds(nested)] = part

    across = {}

    def d_rows(step, pair, other, lo=0, size=own):
        start = place_of_doc(step, pair, other) * own + lo
        return pl.ds(pl.multiple_of(start, half), size)

    def documents_for(step):
        piece = 4 * own
        chip = lax.rem(lax.axis_index("x") + step, chips)
        at = pl.ds(pl.multiple_of(chip * piece, piece), piece)
        product(
            piece,
            lambda nested, cols: contract(
                bands[at, nested * width : (nested + 1) * width], rows_ref[:, cols], 1, 0
            ),
            pd_ref,
            at,
        )
        for pair in (1, 0):
            theirs = pd_ref.at[d_rows(step, pair, 1), :]
            across[step, pair] = send(theirs, sib.at[step * 2 + pair], sibling)

    def queries_at(chip):
        piece = 2 * own
        product(
            piece,
            lambda nested, cols: contract(
                bands[:, pl.ds(pl.multiple_of(nested * width + chip * piece, piece), piece)],
                docs_ref[:, cols],
                0,
                0,
            ),
            pq_ref,
            pl.ds(pl.multiple_of(chip * piece, piece), piece),
        )

    def q_part(step, pair, lo, size, cols):
        start = place_of_row(step, pair) * own + lo
        return pq_ref[pl.ds(pl.multiple_of(start, half), size), cols]

    def d_part(step, pair, lo, size, cols):
        arrive(across[step, pair])
        mine = pd_ref[d_rows(step, pair, 0, lo, size), cols]
        return mine + sib[step * 2 + pair, pl.ds(lo, size), cols]

    waited = []

    def arrive(copy):
        if not any(copy is seen for seen in waited):
            copy.wait_recv()
            waited.append(copy)

    lanes = ((q_part, *neighbours("y")), (d_part, *neighbours("x")))
    edge = split_at(dim)
    early, late = slice(0, edge), slice(edge, dim)
    crossed, far, near = {}, {}, {}

    def cross(which, step):
        part, _, _, pair = lanes[which]
        cross_s[which, step] = part(step, 1, 0, own, late).astype(jnp.bfloat16)
        crossed[which, step] = send(cross_s.at[which, step], cross_r.at[which, step], pair)

    def term(which, pair, cols, step, lo, size):
        value = lanes[which][0](step, pair, lo, size, cols)
        if cols is late:
            arrive(crossed[which, step])
            value = value + cross_r[which, step, pl.ds(lo, size), :].astype(jnp.float32)
        return value

    def send_far(which, pair, cols):
        _, up, down, _ = lanes[which]
        far_s[which, pair, :, cols] = term(which, pair, cols, 2, 0, own).astype(jnp.bfloat16)
        for way, device in ((0, up), (1, down)):
            piece = pl.ds(way * half, half)
            far[which, pair, cols.start, way] = send(
                far_s.at[which, pair, piece, cols], far_r.at[which, pair, piece, cols], device
            )

    def send_near(which, pair, cols):
        _, up, down, _ = lanes[which]
        for way, device, step in ((0, up, 1), (1, down, 3)):
            lo = way * half
            more = half - lo
            near_s[which, pair, way, pl.ds(more, half), cols] = term(
                which, pair, cols, step, more, half
            ).astype(jnp.bfloat16)
            mine = term(which, pair, cols, step, lo, half)
            arrive(far[which, pair, cols.start, way])
            near_s[which, pair, way, pl.ds(lo, half), cols] = (
                mine + far_r[which, pair, pl.ds(lo, half), cols].astype(jnp.float32)
            ).astype(jnp.bfloat16)
            near[which, pair, cols.start, way] = send(
                near_s.at[which, pair, way, :, cols], near_r.at[which, pair, way, :, cols], device
            )

    def summed(which, pair, cols):
        value = term(which, pair, cols, 0, 0, own)
        for way in range(2):
            arrive(near[which, pair, cols.start, way])
            value = value + near_r[which, pair, way, :, cols].astype(jnp.float32)
        return value

    shared = []
    for part in range(2):
        score(part)
        soften(part)
        shared.append(share(part))
    for copy in marked:
        copy.wait_recv()
    partner = jnp.concatenate([marks[place] for place in range(2 * chips)], axis=1)
    band(0, factors(0, shared[0]), partner)
    queries_at(0)
    queries_at(1)
    band(1, factors(1, shared[1]), partner)
    documents_for(2)
    odd = lax.rem(lax.axis_index("y"), 2)
    queries_at(2 + odd)
    cross(0, 2)
    send_far(0, 1, early)
    send_far(0, 0, early)
    queries_at(3 - odd)
    cross(1, 2)
    send_far(1, 1, early)
    send_far(1, 0, early)
    for step in (1, 3, 0):
        cross(0, step)
    documents_for(1)
    documents_for(3)
    for which in range(2):
        send_far(which, 0, late)
    cross(1, 1)
    cross(1, 3)
    for which in range(2):
        send_near(which, 1, early)
    documents_for(0)
    for which in range(2):
        send_near(which, 0, early)
    cross(1, 0)
    for which in range(2):
        send_near(which, 0, late)
    outs = (gq_ref, gd_ref)
    last = []
    for which in range(2):
        pair_s[which] = summed(which, 1, early).astype(jnp.bfloat16)
        last.append(send(pair_s.at[which], pair_r.at[which], lanes[which][3]))
    for which in range(2):
        outs[which][:, early] = summed(which, 0, early)
    for which in range(2):
        outs[which][:, late] = summed(which, 0, late)
    for which in range(2):
        last[which].wait_recv()
        outs[which][:, early] = outs[which][:, early] + pair_r[which].astype(jnp.float32)
    send.finish()


def on_device(queries, documents, partner):
    own, dim = queries.shape
    width, count = 8 * own, 16 * own
    piece = pltpu.VMEM((own, dim), jnp.float32)
    wire = jnp.bfloat16
    edge = split_at(dim)
    copies = 120
    return pl.pallas_call(
        step_kernel,
        out_shape=(piece, piece),
        in_specs=[pl.BlockSpec(memory_space=pl.ANY)] * 2 + [VMEM],
        out_specs=(VMEM, VMEM),
        scratch_shapes=[
            pltpu.VMEM((width, dim), wire),
            pltpu.VMEM((count, dim), wire),
            pltpu.VMEM((WIDTHS, count, width), jnp.float32),
            pltpu.VMEM((count, WIDTHS * width), wire),
            pltpu.VMEM((WIDTHS, 8, width // 2), jnp.float32),
            pltpu.VMEM((WIDTHS, 8, width // 2), jnp.float32),
            pltpu.VMEM((2, 8, width // 2 + 128), jnp.float32),
            pltpu.VMEM((2, 8, width // 2 + 128), jnp.float32),
            pltpu.VMEM((2, 7, 8, width // 2 + 128), jnp.float32),
            pltpu.VMEM((8, 1, own), jnp.int32),
            pltpu.VMEM((width, dim), jnp.float32),
            pltpu.VMEM((count, dim), jnp.float32),
            pltpu.VMEM((8, own, dim), jnp.float32),
            pltpu.VMEM((2, 2, own, dim), wire),
            pltpu.VMEM((2, 2, 2, own, dim), wire),
            pltpu.VMEM((2, 2, own, dim), wire),
            pltpu.VMEM((2, 2, 2, own, dim), wire),
            pltpu.VMEM((2, own, edge), wire),
            pltpu.VMEM((2, own, edge), wire),
            pltpu.VMEM((2, 4, own, dim - edge), wire),
            pltpu.VMEM((2, 4, own, dim - edge), wire),
            pltpu.SemaphoreType.DMA((2,)),
            pltpu.SemaphoreType.DMA((copies,)),
            pltpu.SemaphoreType.DMA((copies,)),
        ],
        compiler_params=pltpu.CompilerParams(
            collective_id=0, has_side_effects=True, vmem_limit_bytes=60 * 2**20
        ),
        name="step",
    )(queries, documents, partner[None, :])


def solution(mesh):
    finer = Mesh(mesh.devices.reshape(4, 2, 4, 2, mesh.shape["rep"]), AXES)
    placed = (P(AXES, None), P(AXES, None), P(AXES))
    return jax.shard_map(
        on_device,
        mesh=finer,
        in_specs=placed,
        out_specs=(P(AXES, None), P(AXES, None)),
        check_vma=False,
    )
```

```python
import functools
import jax
import jax.numpy as jnp
from jax import lax
from jax.experimental import pallas as pl
from jax.experimental.pallas import tpu as pltpu
from jax.sharding import Mesh
from jax.sharding import PartitionSpec as P

WIDTHS = 9
LOG2_E = 1.4426950408889634
logit_gain = 3.0

AXES = ("y", "zl", "x", "core", "zh")
MESH = pl.DeviceIdType.MESH
VMEM = pl.BlockSpec(memory_space=pltpu.VMEM)


def width_list(feature_dim):
    return [feature_dim >> WIDTHS - 1 - nested for nested in range(WIDTHS)]


def split_at(dim):
    return dim * 9 // 16


def contract(first_op, second_op, first_dim, second_dim):
    return lax.dot_general(
        first_op,
        second_op,
        (((first_dim,), (second_dim,)), ((), ())),
        preferred_element_type=jnp.float32,
    )


def neighbours(axis):
    size = lax.axis_size(axis)
    me = lax.axis_index(axis)
    up = {axis: lax.rem(me + 1, size)}
    down = {axis: lax.rem(me + size - 1, size)}
    pair = {"zl": 1 - lax.axis_index("zl")}
    if axis == "x":
        pair["zh"] = 1 - lax.axis_index("zh")
    return up, down, pair


def row_peers():
    chips = lax.axis_size("y")
    y = lax.axis_index("y")
    zl = lax.axis_index("zl")
    return [
        (step, pair, {"y": lax.rem(y + step, chips), "zl": lax.rem(zl + pair, 2)})
        for step in range(chips)
        for pair in range(2)
        if step or pair
    ]


def place_of_row(step, pair):
    y = lax.rem(lax.axis_index("y") + step, lax.axis_size("y"))
    return y * 2 + lax.rem(lax.axis_index("zl") + pair, 2)


def place_of_doc(step, pair, other):
    x = lax.rem(lax.axis_index("x") + step, lax.axis_size("x"))
    zh = lax.rem(lax.axis_index("zh") + pair, 2)
    return (x * 2 + zh) * 2 + lax.rem(lax.axis_index("core") + other, 2)


def first_id(place, own):
    x, there, core = place // 4, lax.rem(place // 2, 2), lax.rem(place, 2)
    zl = lax.rem(lax.axis_index("zl") + lax.axis_index("zh") + there, 2)
    chip = (lax.axis_index("y") * 2 + zl) * lax.axis_size("x") + x
    return ((chip * 2 + core) * 2 + there) * own


def meet(devices):
    barrier = pltpu.get_barrier_semaphore()
    for device in devices:
        pl.semaphore_signal(barrier, inc=1, device_id=device, device_id_type=MESH)
    pl.semaphore_wait(barrier, len(devices))


class Sender:
    def __init__(self, sent, landed):
        self.sent, self.landed, self.started = sent, landed, []

    def __call__(self, src, dst, device):
        number = len(self.started)
        copy = pltpu.make_async_remote_copy(
            src_ref=src,
            dst_ref=dst,
            send_sem=self.sent.at[number],
            recv_sem=self.landed.at[number],
            device_id=device,
            device_id_type=MESH,
        )
        copy.start()
        self.started.append(copy)
        return copy

    def finish(self):
        for copy in self.started:
            copy.wait_send()


def gather(send, rows_ref, docs_ref, own):
    half = own // 2
    sibling = {"core": 1 - lax.axis_index("core")}
    dim = docs_ref.shape[1]
    early, late, every = slice(0, split_at(dim)), slice(split_at(dim), dim), slice(0, dim)

    def q_slot(step, pair, cols, lo=0, size=own):
        start = place_of_row(step, pair) * own + lo
        return rows_ref.at[pl.ds(pl.multiple_of(start, half), size), cols]

    def d_slot(step, pair, cols, lo=0, size=own):
        start = place_of_doc(step, pair, 0) * own + lo
        return docs_ref.at[pl.ds(pl.multiple_of(start, half), size), cols]

    lanes = ((d_slot, *neighbours("x")), (q_slot, *neighbours("y")))
    across = []

    def cross(which, step, pair, cols):
        if which == 0:
            piece = d_slot(step, pair, cols)
            across.append(send(piece, piece, sibling))

    def onward(piece, device):
        return send(piece, piece, device)

    own_early, own_late, up_late, down_late, up_early, down_early = ([] for _ in range(6))
    for slot, up, down, pair in lanes:
        own_early.append(onward(slot(0, 0, early), pair))
        up_late.append(onward(slot(0, 0, late), up))
        down_late.append(onward(slot(0, 0, late), down))
        up_early.append(onward(slot(0, 0, early), up))
        down_early.append(onward(slot(0, 0, early), down))
        own_late.append(onward(slot(0, 0, late), pair))
    cross(0, 0, 0, every)

    def relay(which, step_pair, cols, copies):
        slot, up, down, _ = lanes[which]
        from_down, from_up = copies
        from_down.wait_recv()
        first = onward(slot(3, step_pair, cols, 0, half), up)
        from_up.wait_recv()
        return first, onward(slot(1, step_pair, cols, half, half), down)

    far_late, back_late, beside, far_early, far_pair, last_late = ([] for _ in range(6))
    for which, (slot, up, down, pair) in enumerate(lanes):
        far_late.append(relay(which, 0, late, (up_late[which], down_late[which])))
        back_late.append([onward(slot(step, 0, late), pair) for step in (3, 1)])
    for which, (slot, up, down, pair) in enumerate(lanes):
        own_early[which].wait_recv()
        beside.append([onward(slot(0, 1, early), device) for device in (up, down)])
        cross(which, 0, 1, early)
    for which in range(2):
        far_early.append(relay(which, 0, early, (up_early[which], down_early[which])))
        cross(which, 3, 0, every)
        cross(which, 1, 0, every)
    for which, (slot, up, down, pair) in enumerate(lanes):
        for copy in far_late[which]:
            copy.wait_recv()
        last_late.append(onward(slot(2, 0, late), pair))
        cross(which, 2, 0, late)
        own_late[which].wait_recv()
        cross(which, 0, 1, late)
    for which in range(2):
        far_pair.append(relay(which, 1, early, beside[which]))
        for copy in back_late[which]:
            copy.wait_recv()
        cross(which, 3, 1, every)
        cross(which, 1, 1, every)
    for which in range(2):
        for copy in far_early[which]:
            copy.wait_recv()
        cross(which, 2, 0, early)
    for which in range(2):
        last_late[which].wait_recv()
        cross(which, 2, 1, late)
        for copy in far_pair[which]:
            copy.wait_recv()
        cross(which, 2, 1, early)
    for copy in across:
        copy.wait_recv()


def step_kernel(
    q_ref,
    d_ref,
    p_ref,
    gq_ref,
    gd_ref,
    rows_ref,
    docs_ref,
    logits,
    bands,
    best,
    mass,
    peaks,
    lse,
    parts,
    marks,
    pq_ref,
    pd_ref,
    sib,
    far_s,
    near_s,
    far_r,
    near_r,
    pair_s,
    pair_r,
    cross_s,
    cross_r,
    inside,
    sent,
    landed,
):
    count, dim = docs_ref.shape
    width = rows_ref.shape[0]
    own = q_ref.shape[0]
    half = own // 2
    uppers = width_list(dim)
    lowers = [0] + uppers[:-1]
    scales = [logit_gain * upper ** (-0.5) for upper in uppers]
    narrow = 256
    few = uppers.index(narrow) + 1
    chips = lax.axis_size("y")
    sibling = {"core": 1 - lax.axis_index("core")}
    send = Sender(sent, landed)

    q_place = pl.ds(pl.multiple_of(place_of_row(0, 0) * own, own), own)
    d_place = pl.ds(pl.multiple_of(place_of_doc(0, 0, 0) * own, own), own)
    taken = [
        pltpu.make_async_copy(d_ref, docs_ref.at[d_place, :], inside.at[0]),
        pltpu.make_async_copy(q_ref, rows_ref.at[q_place, :], inside.at[1]),
    ]
    for copy in taken:
        copy.start()
    meet([*neighbours("y"), *neighbours("x"), sibling])
    for copy in taken:
        copy.wait()
    marks[place_of_row(0, 0)] = p_ref[...]
    lse[...] = jnp.zeros_like(lse)
    peaks[...] = jnp.zeros_like(peaks)
    gather(send, rows_ref, docs_ref, own)
    marked = [send(p_ref, marks.at[place_of_row(0, 0)], device) for _, _, device in row_peers()]

    turn = width // 2
    tall = count // 2

    def turn_cols(part, nested=0):
        start = nested * width + part * turn
        return slice(start, start + turn)

    def score(part):
        cols_q = turn_cols(part)
        best[...] = jnp.full(best.shape, -jnp.inf, jnp.float32)

        def keep(nested, at, value):
            logits[nested, at, cols_q] = value
            top = jnp.max(value.reshape(tall // 8, 8, turn), axis=0)
            best[nested] = jnp.maximum(best[nested], top)

        def score_block(block, carry):
            at = pl.ds(pl.multiple_of(block * tall, tall), tall)
            lane = lax.broadcasted_iota(jnp.int32, (tall, narrow), 1)
            head = docs_ref[at, :narrow]
            for nested in range(few):
                cut = jnp.where(lane < uppers[nested], head, jnp.zeros_like(head))
                keep(nested, at, contract(cut, rows_ref[cols_q, :narrow], 1, 1))
            for nested in range(few, WIDTHS):
                cols = slice(lowers[nested], uppers[nested])
                more = contract(docs_ref[at, cols], rows_ref[cols_q, cols], 1, 1)
                keep(nested, at, logits[nested - 1, at, cols_q] + more)
            return carry

        lax.fori_loop(0, count // tall, score_block, 0)

    def soften(part):
        cols_q = turn_cols(part)
        tops = [jnp.max(best[nested], axis=0, keepdims=True) for nested in range(WIDTHS)]
        mass[...] = jnp.zeros_like(mass)
        size = 128

        def mass_block(block, carry):
            at = pl.ds(pl.multiple_of(block * size, size), size)
            for nested in range(WIDTHS):
                piece = logits[nested, at, cols_q] - tops[nested]
                piece = jnp.exp2(piece * (scales[nested] * LOG2_E))
                logits[nested, at, cols_q] = piece
                mass[nested] += jnp.sum(piece.reshape(size // 8, 8, turn), axis=0)
            return carry

        lax.fori_loop(0, count // size, mass_block, 0)
        for nested in range(WIDTHS):
            top = tops[nested] * scales[nested]
            value = top + jnp.log(jnp.sum(mass[nested], axis=0, keepdims=True))
            if nested < 8:
                peaks[part, nested : nested + 1, :turn] = top
                lse[part, nested : nested + 1, :turn] = value
            else:
                for line in range(turn // 128):
                    cols = slice(line * 128, (line + 1) * 128)
                    peaks[part, line : line + 1, turn:] = top[:, cols]
                    lse[part, line : line + 1, turn:] = value[:, cols]

    def share(part):
        return [
            send(lse.at[part], parts.at[part, (chips - step) % chips * 2 + pair - 1], device)
            for step, pair, device in row_peers()
        ]

    def factors(part, copies):
        for copy in copies:
            copy.wait_recv()
        pieces = [lse[part]] + [parts[part, number] for number in range(len(copies))]
        peak = functools.reduce(jnp.maximum, pieces)
        total = peak + jnp.log(sum(jnp.exp(piece - peak) for piece in pieces))
        ratio = jnp.exp(peaks[part] - total)
        rows = [ratio[nested : nested + 1, :turn] * scales[nested] for nested in range(8)]
        tail = [ratio[line : line + 1, turn:] for line in range(turn // 128)]
        return rows + [jnp.concatenate(tail, axis=1) * scales[8]]

    def band(part, factor, partner):
        cols_q = turn_cols(part)

        def band_block(block, carry):
            at = pl.ds(pl.multiple_of(block * own, own), own)
            ids = first_id(block, own) + lax.broadcasted_iota(jnp.int32, (own, turn), 0)
            hit = ids == partner[:, cols_q]
            running = jnp.zeros((own, turn), jnp.float32)
            gone = 0.0
            for nested in reversed(range(WIDTHS)):
                running = running + logits[nested, at, cols_q] * factor[nested]
                gone += scales[nested]
                value = running - jnp.where(hit, gone, 0.0)
                bands[at, turn_cols(part, nested)] = value.astype(jnp.bfloat16)
            return carry

        lax.fori_loop(0, count // own, band_block, 0)

    edge = split_at(dim)
    early, late = slice(0, edge), slice(edge, dim)

    def bounds(nested):
        return slice(0, narrow) if nested < few else slice(lowers[nested], uppers[nested])

    def product(tall_rows, get, out_ref, at):
        lane = lax.broadcasted_iota(jnp.int32, (tall_rows, narrow), 1)
        head = None
        for nested in range(WIDTHS):
            part = get(nested, bounds(nested))
            if nested < few:
                head = part if head is None else jnp.where(lane < lowers[nested], head, part)
                part = head
            if nested >= few - 1:
                out_ref[at, bounds(nested)] = part

    across = {}

    def d_rows(step, pair, other, lo=0, size=own):
        start = place_of_doc(step, pair, other) * own + lo
        return pl.ds(pl.multiple_of(start, half), size)

    def documents_for(step):
        piece = 4 * own
        chip = lax.rem(lax.axis_index("x") + step, chips)
        at = pl.ds(pl.multiple_of(chip * piece, piece), piece)
        product(
            piece,
            lambda nested, cols: contract(
                bands[at, nested * width : (nested + 1) * width], rows_ref[:, cols], 1, 0
            ),
            pd_ref,
            at,
        )
        for pair, cols in ((1, late), (1, early), (0, early), (0, late)):
            across[step, pair, cols.start] = send(
                pd_ref.at[d_rows(step, pair, 1), cols], sib.at[step * 2 + pair, :, cols], sibling
            )

    def queries_at(chip):
        piece = 2 * own
        product(
            piece,
            lambda nested, cols: contract(
                bands[:, pl.ds(pl.multiple_of(nested * width + chip * piece, piece), piece)],
                docs_ref[:, cols],
                0,
                0,
            ),
            pq_ref,
            pl.ds(pl.multiple_of(chip * piece, piece), piece),
        )

    def q_part(step, pair, lo, size, cols):
        start = place_of_row(step, pair) * own + lo
        return pq_ref[pl.ds(pl.multiple_of(start, half), size), cols]

    def d_part(step, pair, lo, size, cols):
        arrive(across[step, pair, cols.start])
        mine = pd_ref[d_rows(step, pair, 0, lo, size), cols]
        return mine + sib[step * 2 + pair, pl.ds(lo, size), cols]

    waited = []

    def arrive(copy):
        if not any(copy is seen for seen in waited):
            copy.wait_recv()
            waited.append(copy)

    lanes = ((q_part, *neighbours("y")), (d_part, *neighbours("x")))
    crossed, far, near = {}, {}, {}

    def cross(which, step):
        part, _, _, pair = lanes[which]
        cross_s[which, step] = part(step, 1, 0, own, late).astype(jnp.bfloat16)
        crossed[which, step] = send(cross_s.at[which, step], cross_r.at[which, step], pair)

    def term(which, pair, cols, step, lo, size):
        value = lanes[which][0](step, pair, lo, size, cols)
        if cols is late:
            arrive(crossed[which, step])
            value = value + cross_r[which, step, pl.ds(lo, size), :].astype(jnp.float32)
        return value

    def send_far(which, pair, cols):
        _, up, down, _ = lanes[which]
        far_s[which, pair, :, cols] = term(which, pair, cols, 2, 0, own).astype(jnp.bfloat16)
        for way, device in ((0, up), (1, down)):
            piece = pl.ds(way * half, half)
            far[which, pair, cols.start, way] = send(
                far_s.at[which, pair, piece, cols], far_r.at[which, pair, piece, cols], device
            )

    def send_near(which, pair, cols):
        _, up, down, _ = lanes[which]
        for way, device, step in ((0, up, 1), (1, down, 3)):
            lo = way * half
            more = half - lo
            near_s[which, pair, way, pl.ds(more, half), cols] = term(
                which, pair, cols, step, more, half
            ).astype(jnp.bfloat16)
            mine = term(which, pair, cols, step, lo, half)
            arrive(far[which, pair, cols.start, way])
            near_s[which, pair, way, pl.ds(lo, half), cols] = (
                mine + far_r[which, pair, pl.ds(lo, half), cols].astype(jnp.float32)
            ).astype(jnp.bfloat16)
            near[which, pair, cols.start, way] = send(
                near_s.at[which, pair, way, :, cols], near_r.at[which, pair, way, :, cols], device
            )

    def summed(which, pair, cols):
        value = term(which, pair, cols, 0, 0, own)
        for way in range(2):
            arrive(near[which, pair, cols.start, way])
            value = value + near_r[which, pair, way, :, cols].astype(jnp.float32)
        return value

    shared = []
    for part in range(2):
        score(part)
        soften(part)
        shared.append(share(part))
    for copy in marked:
        copy.wait_recv()
    partner = jnp.concatenate([marks[place] for place in range(2 * chips)], axis=1)
    band(0, factors(0, shared[0]), partner)
    queries_at(0)
    queries_at(1)
    band(1, factors(1, shared[1]), partner)
    documents_for(2)
    odd = lax.rem(lax.axis_index("y"), 2)
    queries_at(2 + odd)
    cross(0, 2)
    send_far(0, 1, early)
    send_far(0, 0, early)
    cross(0, 0)
    documents_for(1)
    cross(1, 2)
    send_far(1, 1, early)
    send_far(1, 0, early)
    documents_for(3)
    cross(1, 1)
    queries_at(3 - odd)
    cross(1, 3)
    cross(0, 1)
    cross(0, 3)
    send_near(0, 1, early)
    send_far(0, 0, late)
    send_near(1, 1, early)
    send_far(1, 0, late)
    documents_for(0)
    cross(1, 0)
    for which in (0, 1):
        send_near(which, 0, early)
    for which in (0, 1):
        send_near(which, 0, late)
    outs = (gq_ref, gd_ref)
    last = []
    for which in range(2):
        pair_s[which] = summed(which, 1, early).astype(jnp.bfloat16)
        last.append(send(pair_s.at[which], pair_r.at[which], lanes[which][3]))
    for which in range(2):
        outs[which][:, early] = summed(which, 0, early)
    for which in range(2):
        outs[which][:, late] = summed(which, 0, late)
    for which in range(2):
        last[which].wait_recv()
        outs[which][:, early] = outs[which][:, early] + pair_r[which].astype(jnp.float32)
    send.finish()


def on_device(queries, documents, partner):
    own, dim = queries.shape
    width, count = 8 * own, 16 * own
    piece = pltpu.VMEM((own, dim), jnp.float32)
    wire = jnp.bfloat16
    edge = split_at(dim)
    copies = 120
    return pl.pallas_call(
        step_kernel,
        out_shape=(piece, piece),
        in_specs=[pl.BlockSpec(memory_space=pl.ANY)] * 2 + [VMEM],
        out_specs=(VMEM, VMEM),
        scratch_shapes=[
            pltpu.VMEM((width, dim), wire),
            pltpu.VMEM((count, dim), wire),
            pltpu.VMEM((WIDTHS, count, width), jnp.float32),
            pltpu.VMEM((count, WIDTHS * width), wire),
            pltpu.VMEM((WIDTHS, 8, width // 2), jnp.float32),
            pltpu.VMEM((WIDTHS, 8, width // 2), jnp.float32),
            pltpu.VMEM((2, 8, width // 2 + 128), jnp.float32),
            pltpu.VMEM((2, 8, width // 2 + 128), jnp.float32),
            pltpu.VMEM((2, 7, 8, width // 2 + 128), jnp.float32),
            pltpu.VMEM((8, 1, own), jnp.int32),
            pltpu.VMEM((width, dim), jnp.float32),
            pltpu.VMEM((count, dim), jnp.float32),
            pltpu.VMEM((8, own, dim), jnp.float32),
            pltpu.VMEM((2, 2, own, dim), wire),
            pltpu.VMEM((2, 2, 2, own, dim), wire),
            pltpu.VMEM((2, 2, own, dim), wire),
            pltpu.VMEM((2, 2, 2, own, dim), wire),
            pltpu.VMEM((2, own, edge), wire),
            pltpu.VMEM((2, own, edge), wire),
            pltpu.VMEM((2, 4, own, dim - edge), wire),
            pltpu.VMEM((2, 4, own, dim - edge), wire),
            pltpu.SemaphoreType.DMA((2,)),
            pltpu.SemaphoreType.DMA((copies,)),
            pltpu.SemaphoreType.DMA((copies,)),
        ],
        compiler_params=pltpu.CompilerParams(
            collective_id=0, has_side_effects=True, vmem_limit_bytes=60 * 2**20
        ),
        name="step",
    )(queries, documents, partner[None, :])


def solution(mesh):
    finer = Mesh(mesh.devices.reshape(4, 2, 4, 2, mesh.shape["rep"]), AXES)
    placed = (P(AXES, None), P(AXES, None), P(AXES))
    return jax.shard_map(
        on_device,
        mesh=finer,
        in_specs=placed,
        out_specs=(P(AXES, None), P(AXES, None)),
        check_vma=False,
    )
```

```python
import functools
import jax
import jax.numpy as jnp
from jax import lax
from jax.experimental import pallas as pl
from jax.experimental.pallas import tpu as pltpu
from jax.sharding import Mesh
from jax.sharding import PartitionSpec as P

WIDTHS = 9
LOG2_E = 1.4426950408889634
logit_gain = 3.0

AXES = ("y", "zl", "x", "core", "zh")
MESH = pl.DeviceIdType.MESH
VMEM = pl.BlockSpec(memory_space=pltpu.VMEM)


def width_list(feature_dim):
    return [feature_dim >> WIDTHS - 1 - nested for nested in range(WIDTHS)]


def split_at(dim):
    return dim * 9 // 16


def contract(first_op, second_op, first_dim, second_dim):
    return lax.dot_general(
        first_op,
        second_op,
        (((first_dim,), (second_dim,)), ((), ())),
        preferred_element_type=jnp.float32,
    )


def neighbours(axis):
    size = lax.axis_size(axis)
    me = lax.axis_index(axis)
    up = {axis: lax.rem(me + 1, size)}
    down = {axis: lax.rem(me + size - 1, size)}
    pair = {"zl": 1 - lax.axis_index("zl")}
    if axis == "x":
        pair["zh"] = 1 - lax.axis_index("zh")
    return up, down, pair


def row_peers():
    chips = lax.axis_size("y")
    y = lax.axis_index("y")
    zl = lax.axis_index("zl")
    return [
        (step, pair, {"y": lax.rem(y + step, chips), "zl": lax.rem(zl + pair, 2)})
        for step in range(chips)
        for pair in range(2)
        if step or pair
    ]


def place_of_row(step, pair):
    y = lax.rem(lax.axis_index("y") + step, lax.axis_size("y"))
    return y * 2 + lax.rem(lax.axis_index("zl") + pair, 2)


def place_of_doc(step, pair, other):
    x = lax.rem(lax.axis_index("x") + step, lax.axis_size("x"))
    zh = lax.rem(lax.axis_index("zh") + pair, 2)
    return (x * 2 + zh) * 2 + lax.rem(lax.axis_index("core") + other, 2)


def first_id(place, own):
    x, there, core = place // 4, lax.rem(place // 2, 2), lax.rem(place, 2)
    zl = lax.rem(lax.axis_index("zl") + lax.axis_index("zh") + there, 2)
    chip = (lax.axis_index("y") * 2 + zl) * lax.axis_size("x") + x
    return ((chip * 2 + core) * 2 + there) * own


def meet(devices):
    barrier = pltpu.get_barrier_semaphore()
    for device in devices:
        pl.semaphore_signal(barrier, inc=1, device_id=device, device_id_type=MESH)
    pl.semaphore_wait(barrier, len(devices))


class Sender:
    def __init__(self, sent, landed):
        self.sent, self.landed, self.started = sent, landed, []

    def __call__(self, src, dst, device):
        number = len(self.started)
        copy = pltpu.make_async_remote_copy(
            src_ref=src,
            dst_ref=dst,
            send_sem=self.sent.at[number],
            recv_sem=self.landed.at[number],
            device_id=device,
            device_id_type=MESH,
        )
        copy.start()
        self.started.append(copy)
        return copy

    def finish(self):
        for copy in self.started:
            copy.wait_send()


def gather(send, rows_ref, docs_ref, own):
    half = own // 2
    sibling = {"core": 1 - lax.axis_index("core")}
    dim = docs_ref.shape[1]
    early, late, every = slice(0, split_at(dim)), slice(split_at(dim), dim), slice(0, dim)

    def q_slot(step, pair, cols, lo=0, size=own):
        start = place_of_row(step, pair) * own + lo
        return rows_ref.at[pl.ds(pl.multiple_of(start, half), size), cols]

    def d_slot(step, pair, cols, lo=0, size=own):
        start = place_of_doc(step, pair, 0) * own + lo
        return docs_ref.at[pl.ds(pl.multiple_of(start, half), size), cols]

    lanes = ((d_slot, *neighbours("x")), (q_slot, *neighbours("y")))
    across = []

    def cross(which, step, pair, cols):
        if which == 0:
            piece = d_slot(step, pair, cols)
            across.append(send(piece, piece, sibling))

    def onward(piece, device):
        return send(piece, piece, device)

    own_early, own_late, up_late, down_late, up_early, down_early = ([] for _ in range(6))
    for slot, up, down, pair in lanes:
        own_early.append(onward(slot(0, 0, early), pair))
        up_late.append(onward(slot(0, 0, late), up))
        down_late.append(onward(slot(0, 0, late), down))
        up_early.append(onward(slot(0, 0, early), up))
        down_early.append(onward(slot(0, 0, early), down))
        own_late.append(onward(slot(0, 0, late), pair))
    cross(0, 0, 0, every)

    def relay(which, step_pair, cols, copies):
        slot, up, down, _ = lanes[which]
        from_down, from_up = copies
        from_down.wait_recv()
        first = onward(slot(3, step_pair, cols, 0, half), up)
        from_up.wait_recv()
        return first, onward(slot(1, step_pair, cols, half, half), down)

    far_late, back_late, beside, far_early, far_pair, last_late = ([] for _ in range(6))
    for which, (slot, up, down, pair) in enumerate(lanes):
        far_late.append(relay(which, 0, late, (up_late[which], down_late[which])))
        back_late.append([onward(slot(step, 0, late), pair) for step in (3, 1)])
    for which, (slot, up, down, pair) in enumerate(lanes):
        own_early[which].wait_recv()
        beside.append([onward(slot(0, 1, early), device) for device in (up, down)])
        cross(which, 0, 1, early)
    for which in range(2):
        far_early.append(relay(which, 0, early, (up_early[which], down_early[which])))
        cross(which, 3, 0, every)
        cross(which, 1, 0, every)
    for which, (slot, up, down, pair) in enumerate(lanes):
        for copy in far_late[which]:
            copy.wait_recv()
        last_late.append(onward(slot(2, 0, late), pair))
        cross(which, 2, 0, late)
        own_late[which].wait_recv()
        cross(which, 0, 1, late)
    for which in range(2):
        far_pair.append(relay(which, 1, early, beside[which]))
        for copy in back_late[which]:
            copy.wait_recv()
        cross(which, 3, 1, every)
        cross(which, 1, 1, every)
    for which in range(2):
        for copy in far_early[which]:
            copy.wait_recv()
        cross(which, 2, 0, early)
    for which in range(2):
        last_late[which].wait_recv()
        cross(which, 2, 1, late)
        for copy in far_pair[which]:
            copy.wait_recv()
        cross(which, 2, 1, early)
    for copy in across:
        copy.wait_recv()


def step_kernel(
    q_ref,
    d_ref,
    p_ref,
    gq_ref,
    gd_ref,
    rows_ref,
    docs_ref,
    logits,
    bands,
    best,
    mass,
    peaks,
    lse,
    parts,
    marks,
    pq_ref,
    pd_ref,
    sib,
    far_s,
    near_s,
    far_r,
    near_r,
    pair_s,
    pair_r,
    cross_s,
    cross_r,
    inside,
    sent,
    landed,
):
    count, dim = docs_ref.shape
    width = rows_ref.shape[0]
    own = q_ref.shape[0]
    half = own // 2
    uppers = width_list(dim)
    lowers = [0] + uppers[:-1]
    scales = [logit_gain * upper ** (-0.5) for upper in uppers]
    narrow = 256
    few = uppers.index(narrow) + 1
    chips = lax.axis_size("y")
    sibling = {"core": 1 - lax.axis_index("core")}
    send = Sender(sent, landed)

    q_place = pl.ds(pl.multiple_of(place_of_row(0, 0) * own, own), own)
    d_place = pl.ds(pl.multiple_of(place_of_doc(0, 0, 0) * own, own), own)
    taken = [
        pltpu.make_async_copy(d_ref, docs_ref.at[d_place, :], inside.at[0]),
        pltpu.make_async_copy(q_ref, rows_ref.at[q_place, :], inside.at[1]),
        pltpu.make_async_copy(p_ref, marks.at[place_of_row(0, 0)], inside.at[2]),
    ]
    for copy in taken:
        copy.start()
    meet([*neighbours("y"), *neighbours("x"), sibling])
    for copy in taken:
        copy.wait()
    lse[...] = jnp.zeros_like(lse)
    peaks[...] = jnp.zeros_like(peaks)
    gather(send, rows_ref, docs_ref, own)
    mark = marks.at[place_of_row(0, 0)]
    marked = [send(mark, mark, device) for _, _, device in row_peers()]

    turn = width // 2
    tall = count // 2

    def turn_cols(part, nested=0):
        start = nested * width + part * turn
        return slice(start, start + turn)

    def score(part):
        cols_q = turn_cols(part)
        best[...] = jnp.full(best.shape, -jnp.inf, jnp.float32)

        def keep(nested, at, value):
            logits[nested, at, cols_q] = value
            top = jnp.max(value.reshape(tall // 8, 8, turn), axis=0)
            best[nested] = jnp.maximum(best[nested], top)

        def score_block(block, carry):
            at = pl.ds(pl.multiple_of(block * tall, tall), tall)
            lane = lax.broadcasted_iota(jnp.int32, (tall, narrow), 1)
            head = docs_ref[at, :narrow]
            for nested in range(few):
                cut = jnp.where(lane < uppers[nested], head, jnp.zeros_like(head))
                keep(nested, at, contract(cut, rows_ref[cols_q, :narrow], 1, 1))
            for nested in range(few, WIDTHS):
                cols = slice(lowers[nested], uppers[nested])
                more = contract(docs_ref[at, cols], rows_ref[cols_q, cols], 1, 1)
                keep(nested, at, logits[nested - 1, at, cols_q] + more)
            return carry

        lax.fori_loop(0, count // tall, score_block, 0)

    def soften(part):
        cols_q = turn_cols(part)
        tops = [jnp.max(best[nested], axis=0, keepdims=True) for nested in range(WIDTHS)]
        mass[...] = jnp.zeros_like(mass)
        size = 128

        def mass_block(block, carry):
            at = pl.ds(pl.multiple_of(block * size, size), size)
            for nested in range(WIDTHS):
                piece = logits[nested, at, cols_q] - tops[nested]
                piece = jnp.exp2(piece * (scales[nested] * LOG2_E))
                logits[nested, at, cols_q] = piece
                mass[nested] += jnp.sum(piece.reshape(size // 8, 8, turn), axis=0)
            return carry

        lax.fori_loop(0, count // size, mass_block, 0)
        for nested in range(WIDTHS):
            top = tops[nested] * scales[nested]
            value = top + jnp.log(jnp.sum(mass[nested], axis=0, keepdims=True))
            if nested < 8:
                peaks[part, nested : nested + 1, :turn] = top
                lse[part, nested : nested + 1, :turn] = value
            else:
                for line in range(turn // 128):
                    cols = slice(line * 128, (line + 1) * 128)
                    peaks[part, line : line + 1, turn:] = top[:, cols]
                    lse[part, line : line + 1, turn:] = value[:, cols]

    def share(part):
        return [
            send(lse.at[part], parts.at[part, (chips - step) % chips * 2 + pair - 1], device)
            for step, pair, device in row_peers()
        ]

    def factors(part, copies):
        for copy in copies:
            copy.wait_recv()
        pieces = [lse[part]] + [parts[part, number] for number in range(len(copies))]
        peak = functools.reduce(jnp.maximum, pieces)
        total = peak + jnp.log(sum(jnp.exp(piece - peak) for piece in pieces))
        ratio = jnp.exp(peaks[part] - total)
        rows = [ratio[nested : nested + 1, :turn] * scales[nested] for nested in range(8)]
        tail = [ratio[line : line + 1, turn:] for line in range(turn // 128)]
        return rows + [jnp.concatenate(tail, axis=1) * scales[8]]

    def band(part, factor, partner):
        cols_q = turn_cols(part)

        def band_block(block, carry):
            at = pl.ds(pl.multiple_of(block * own, own), own)
            ids = first_id(block, own) + lax.broadcasted_iota(jnp.int32, (own, turn), 0)
            hit = ids == partner[:, cols_q]
            running = jnp.zeros((own, turn), jnp.float32)
            gone = 0.0
            for nested in reversed(range(WIDTHS)):
                running = running + logits[nested, at, cols_q] * factor[nested]
                gone += scales[nested]
                value = running - jnp.where(hit, gone, 0.0)
                bands[at, turn_cols(part, nested)] = value.astype(jnp.bfloat16)
            return carry

        lax.fori_loop(0, count // own, band_block, 0)

    edge = split_at(dim)
    early, late = slice(0, edge), slice(edge, dim)

    def bounds(nested):
        return slice(0, narrow) if nested < few else slice(lowers[nested], uppers[nested])

    def product(tall_rows, get, out_ref, at):
        lane = lax.broadcasted_iota(jnp.int32, (tall_rows, narrow), 1)
        head = None
        for nested in range(WIDTHS):
            part = get(nested, bounds(nested))
            if nested < few:
                head = part if head is None else jnp.where(lane < lowers[nested], head, part)
                part = head
            if nested >= few - 1:
                out_ref[at, bounds(nested)] = part

    across = {}

    def d_rows(step, pair, other, lo=0, size=own):
        start = place_of_doc(step, pair, other) * own + lo
        return pl.ds(pl.multiple_of(start, half), size)

    def documents_for(step):
        piece = 4 * own
        chip = lax.rem(lax.axis_index("x") + step, chips)
        at = pl.ds(pl.multiple_of(chip * piece, piece), piece)
        product(
            piece,
            lambda nested, cols: contract(
                bands[at, nested * width : (nested + 1) * width], rows_ref[:, cols], 1, 0
            ),
            pd_ref,
            at,
        )
        for pair, cols in ((1, late), (1, early), (0, early), (0, late)):
            across[step, pair, cols.start] = send(
                pd_ref.at[d_rows(step, pair, 1), cols], sib.at[step * 2 + pair, :, cols], sibling
            )

    def queries_at(chip):
        piece = 2 * own
        product(
            piece,
            lambda nested, cols: contract(
                bands[:, pl.ds(pl.multiple_of(nested * width + chip * piece, piece), piece)],
                docs_ref[:, cols],
                0,
                0,
            ),
            pq_ref,
            pl.ds(pl.multiple_of(chip * piece, piece), piece),
        )

    def q_part(step, pair, lo, size, cols):
        start = place_of_row(step, pair) * own + lo
        return pq_ref[pl.ds(pl.multiple_of(start, half), size), cols]

    def d_part(step, pair, lo, size, cols):
        arrive(across[step, pair, cols.start])
        mine = pd_ref[d_rows(step, pair, 0, lo, size), cols]
        return mine + sib[step * 2 + pair, pl.ds(lo, size), cols]

    waited = []

    def arrive(copy):
        if not any(copy is seen for seen in waited):
            copy.wait_recv()
            waited.append(copy)

    lanes = ((q_part, *neighbours("y")), (d_part, *neighbours("x")))
    crossed, far, near = {}, {}, {}

    def cross(which, step):
        part, _, _, pair = lanes[which]
        cross_s[which, step] = part(step, 1, 0, own, late).astype(jnp.bfloat16)
        crossed[which, step] = send(cross_s.at[which, step], cross_r.at[which, step], pair)

    def term(which, pair, cols, step, lo, size):
        value = lanes[which][0](step, pair, lo, size, cols)
        if cols is late:
            arrive(crossed[which, step])
            value = value + cross_r[which, step, pl.ds(lo, size), :].astype(jnp.float32)
        return value

    def send_far(which, pair, cols):
        _, up, down, _ = lanes[which]
        far_s[which, pair, :, cols] = term(which, pair, cols, 2, 0, own).astype(jnp.bfloat16)
        for way, device in ((0, up), (1, down)):
            piece = pl.ds(way * half, half)
            far[which, pair, cols.start, way] = send(
                far_s.at[which, pair, piece, cols], far_r.at[which, pair, piece, cols], device
            )

    def send_near(which, pair, cols):
        _, up, down, _ = lanes[which]
        for way, device, step in ((0, up, 1), (1, down, 3)):
            lo = way * half
            more = half - lo
            near_s[which, pair, way, pl.ds(more, half), cols] = term(
                which, pair, cols, step, more, half
            ).astype(jnp.bfloat16)
            mine = term(which, pair, cols, step, lo, half)
            arrive(far[which, pair, cols.start, way])
            near_s[which, pair, way, pl.ds(lo, half), cols] = (
                mine + far_r[which, pair, pl.ds(lo, half), cols].astype(jnp.float32)
            ).astype(jnp.bfloat16)
            near[which, pair, cols.start, way] = send(
                near_s.at[which, pair, way, :, cols], near_r.at[which, pair, way, :, cols], device
            )

    def summed(which, pair, cols):
        value = term(which, pair, cols, 0, 0, own)
        for way in range(2):
            arrive(near[which, pair, cols.start, way])
            value = value + near_r[which, pair, way, :, cols].astype(jnp.float32)
        return value

    shared = []
    for part in range(2):
        score(part)
        soften(part)
        shared.append(share(part))
    for copy in marked:
        copy.wait_recv()
    partner = jnp.concatenate([marks[place] for place in range(2 * chips)], axis=1)
    band(0, factors(0, shared[0]), partner)
    queries_at(0)
    queries_at(1)
    band(1, factors(1, shared[1]), partner)
    documents_for(2)
    odd = lax.rem(lax.axis_index("y"), 2)
    queries_at(2 + odd)
    cross(0, 2)
    send_far(0, 1, early)
    send_far(0, 0, early)
    cross(0, 0)
    documents_for(1)
    cross(1, 2)
    send_far(1, 1, early)
    send_far(1, 0, early)
    documents_for(3)
    cross(1, 1)
    queries_at(3 - odd)
    cross(1, 3)
    cross(0, 1)
    cross(0, 3)
    send_near(0, 1, early)
    send_far(0, 0, late)
    send_near(1, 1, early)
    send_far(1, 0, late)
    documents_for(0)
    cross(1, 0)
    for which in (0, 1):
        send_near(which, 0, early)
    for which in (0, 1):
        send_near(which, 0, late)
    outs = (gq_ref, gd_ref)
    last = []
    for which in range(2):
        pair_s[which] = summed(which, 1, early).astype(jnp.bfloat16)
        last.append(send(pair_s.at[which], pair_r.at[which], lanes[which][3]))
    for which in range(2):
        outs[which][:, early] = summed(which, 0, early)
    for which in range(2):
        outs[which][:, late] = summed(which, 0, late)
    for which in range(2):
        last[which].wait_recv()
        outs[which][:, early] = outs[which][:, early] + pair_r[which].astype(jnp.float32)
    send.finish()


def on_device(queries, documents, partner):
    own, dim = queries.shape
    width, count = 8 * own, 16 * own
    piece = pltpu.VMEM((own, dim), jnp.float32)
    wire = jnp.bfloat16
    edge = split_at(dim)
    copies = 120
    return pl.pallas_call(
        step_kernel,
        out_shape=(piece, piece),
        in_specs=[pl.BlockSpec(memory_space=pl.ANY)] * 3,
        out_specs=(VMEM, VMEM),
        scratch_shapes=[
            pltpu.VMEM((width, dim), wire),
            pltpu.VMEM((count, dim), wire),
            pltpu.VMEM((WIDTHS, count, width), jnp.float32),
            pltpu.VMEM((count, WIDTHS * width), wire),
            pltpu.VMEM((WIDTHS, 8, width // 2), jnp.float32),
            pltpu.VMEM((WIDTHS, 8, width // 2), jnp.float32),
            pltpu.VMEM((2, 8, width // 2 + 128), jnp.float32),
            pltpu.VMEM((2, 8, width // 2 + 128), jnp.float32),
            pltpu.VMEM((2, 7, 8, width // 2 + 128), jnp.float32),
            pltpu.VMEM((8, 1, own), jnp.int32),
            pltpu.VMEM((width, dim), jnp.float32),
            pltpu.VMEM((count, dim), jnp.float32),
            pltpu.VMEM((8, own, dim), jnp.float32),
            pltpu.VMEM((2, 2, own, dim), wire),
            pltpu.VMEM((2, 2, 2, own, dim), wire),
            pltpu.VMEM((2, 2, own, dim), wire),
            pltpu.VMEM((2, 2, 2, own, dim), wire),
            pltpu.VMEM((2, own, edge), wire),
            pltpu.VMEM((2, own, edge), wire),
            pltpu.VMEM((2, 4, own, dim - edge), wire),
            pltpu.VMEM((2, 4, own, dim - edge), wire),
            pltpu.SemaphoreType.DMA((3,)),
            pltpu.SemaphoreType.DMA((copies,)),
            pltpu.SemaphoreType.DMA((copies,)),
        ],
        compiler_params=pltpu.CompilerParams(
            collective_id=0, has_side_effects=True, vmem_limit_bytes=60 * 2**20
        ),
        name="step",
    )(queries, documents, partner[None, :])


def solution(mesh):
    finer = Mesh(mesh.devices.reshape(4, 2, 4, 2, mesh.shape["rep"]), AXES)
    placed = (P(AXES, None), P(AXES, None), P(AXES))
    return jax.shard_map(
        on_device,
        mesh=finer,
        in_specs=placed,
        out_specs=(P(AXES, None), P(AXES, None)),
        check_vma=False,
    )
```

```python
import functools
import jax
import jax.numpy as jnp
from jax import lax
from jax.experimental import pallas as pl
from jax.experimental.pallas import tpu as pltpu
from jax.sharding import Mesh
from jax.sharding import PartitionSpec as P

WIDTHS = 9
LOG2_E = 1.4426950408889634
logit_gain = 3.0

AXES = ("y", "zl", "x", "core", "zh")
MESH = pl.DeviceIdType.MESH
VMEM = pl.BlockSpec(memory_space=pltpu.VMEM)


def width_list(feature_dim):
    return [feature_dim >> WIDTHS - 1 - nested for nested in range(WIDTHS)]


def split_at(dim):
    return dim * 9 // 16


def contract(first_op, second_op, first_dim, second_dim):
    return lax.dot_general(
        first_op,
        second_op,
        (((first_dim,), (second_dim,)), ((), ())),
        preferred_element_type=jnp.float32,
    )


def neighbours(axis):
    size = lax.axis_size(axis)
    me = lax.axis_index(axis)
    up = {axis: lax.rem(me + 1, size)}
    down = {axis: lax.rem(me + size - 1, size)}
    pair = {"zl": 1 - lax.axis_index("zl")}
    if axis == "x":
        pair["zh"] = 1 - lax.axis_index("zh")
    return up, down, pair


def row_peers():
    chips = lax.axis_size("y")
    y = lax.axis_index("y")
    zl = lax.axis_index("zl")
    return [
        (step, pair, {"y": lax.rem(y + step, chips), "zl": lax.rem(zl + pair, 2)})
        for step in range(chips)
        for pair in range(2)
        if step or pair
    ]


def place_of_row(step, pair):
    y = lax.rem(lax.axis_index("y") + step, lax.axis_size("y"))
    return y * 2 + lax.rem(lax.axis_index("zl") + pair, 2)


def place_of_doc(step, pair, other):
    x = lax.rem(lax.axis_index("x") + step, lax.axis_size("x"))
    zh = lax.rem(lax.axis_index("zh") + pair, 2)
    return (x * 2 + zh) * 2 + lax.rem(lax.axis_index("core") + other, 2)


def first_id(place, own):
    x, there, core = place // 4, lax.rem(place // 2, 2), lax.rem(place, 2)
    zl = lax.rem(lax.axis_index("zl") + lax.axis_index("zh") + there, 2)
    chip = (lax.axis_index("y") * 2 + zl) * lax.axis_size("x") + x
    return ((chip * 2 + core) * 2 + there) * own


def meet(devices):
    barrier = pltpu.get_barrier_semaphore()
    for device in devices:
        pl.semaphore_signal(barrier, inc=1, device_id=device, device_id_type=MESH)
    pl.semaphore_wait(barrier, len(devices))


class Sender:
    def __init__(self, sent, landed):
        self.sent, self.landed, self.started = sent, landed, []

    def __call__(self, src, dst, device):
        number = len(self.started)
        copy = pltpu.make_async_remote_copy(
            src_ref=src,
            dst_ref=dst,
            send_sem=self.sent.at[number],
            recv_sem=self.landed.at[number],
            device_id=device,
            device_id_type=MESH,
        )
        copy.start()
        self.started.append(copy)
        return copy

    def finish(self):
        for copy in self.started:
            copy.wait_send()


def gather(send, rows_ref, docs_ref, own):
    half = own // 2
    sibling = {"core": 1 - lax.axis_index("core")}
    dim = docs_ref.shape[1]
    early, late, every = slice(0, split_at(dim)), slice(split_at(dim), dim), slice(0, dim)

    def q_slot(step, pair, cols, lo=0, size=own):
        start = place_of_row(step, pair) * own + lo
        return rows_ref.at[pl.ds(pl.multiple_of(start, half), size), cols]

    def d_slot(step, pair, cols, lo=0, size=own):
        start = place_of_doc(step, pair, 0) * own + lo
        return docs_ref.at[pl.ds(pl.multiple_of(start, half), size), cols]

    lanes = ((d_slot, *neighbours("x")), (q_slot, *neighbours("y")))
    across = []

    def cross(which, step, pair, cols):
        if which == 0:
            piece = d_slot(step, pair, cols)
            across.append(send(piece, piece, sibling))

    def onward(piece, device):
        return send(piece, piece, device)

    own_early, own_late, up_late, down_late, up_early, down_early = ([] for _ in range(6))
    for slot, up, down, pair in lanes:
        own_early.append(onward(slot(0, 0, early), pair))
        up_late.append(onward(slot(0, 0, late), up))
        down_late.append(onward(slot(0, 0, late), down))
        up_early.append(onward(slot(0, 0, early), up))
        down_early.append(onward(slot(0, 0, early), down))
        own_late.append(onward(slot(0, 0, late), pair))
    cross(0, 0, 0, every)

    def relay(which, step_pair, cols, copies):
        slot, up, down, _ = lanes[which]
        from_down, from_up = copies
        from_down.wait_recv()
        first = onward(slot(3, step_pair, cols, 0, half), up)
        from_up.wait_recv()
        return first, onward(slot(1, step_pair, cols, half, half), down)

    far_late, back_late, beside, far_early, far_pair, last_late = ([] for _ in range(6))
    for which, (slot, up, down, pair) in enumerate(lanes):
        far_late.append(relay(which, 0, late, (up_late[which], down_late[which])))
        back_late.append([onward(slot(step, 0, late), pair) for step in (3, 1)])
    for which, (slot, up, down, pair) in enumerate(lanes):
        own_early[which].wait_recv()
        beside.append([onward(slot(0, 1, early), device) for device in (up, down)])
        cross(which, 0, 1, early)
    for which in range(2):
        far_early.append(relay(which, 0, early, (up_early[which], down_early[which])))
        cross(which, 3, 0, every)
        cross(which, 1, 0, every)
    for which, (slot, up, down, pair) in enumerate(lanes):
        for copy in far_late[which]:
            copy.wait_recv()
        last_late.append(onward(slot(2, 0, late), pair))
        cross(which, 2, 0, late)
        own_late[which].wait_recv()
        cross(which, 0, 1, late)
    for which in range(2):
        far_pair.append(relay(which, 1, early, beside[which]))
        for copy in back_late[which]:
            copy.wait_recv()
        cross(which, 3, 1, every)
        cross(which, 1, 1, every)
    for which in range(2):
        for copy in far_early[which]:
            copy.wait_recv()
        cross(which, 2, 0, early)
    for which in range(2):
        last_late[which].wait_recv()
        cross(which, 2, 1, late)
        for copy in far_pair[which]:
            copy.wait_recv()
        cross(which, 2, 1, early)
    for copy in across:
        copy.wait_recv()


def step_kernel(
    q_ref,
    d_ref,
    p_ref,
    gq_ref,
    gd_ref,
    rows_ref,
    docs_ref,
    logits,
    bands,
    best,
    mass,
    peaks,
    lse,
    parts,
    marks,
    pq_ref,
    pd_ref,
    sib,
    far_s,
    near_s,
    far_r,
    near_r,
    pair_s,
    pair_r,
    cross_s,
    cross_r,
    inside,
    sent,
    landed,
):
    count, dim = docs_ref.shape
    width = rows_ref.shape[0]
    own = q_ref.shape[0]
    half = own // 2
    uppers = width_list(dim)
    lowers = [0] + uppers[:-1]
    scales = [logit_gain * upper ** (-0.5) for upper in uppers]
    narrow = 256
    few = uppers.index(narrow) + 1
    chips = lax.axis_size("y")
    sibling = {"core": 1 - lax.axis_index("core")}
    send = Sender(sent, landed)

    q_place = pl.ds(pl.multiple_of(place_of_row(0, 0) * own, own), own)
    d_place = pl.ds(pl.multiple_of(place_of_doc(0, 0, 0) * own, own), own)
    taken = [
        pltpu.make_async_copy(d_ref, docs_ref.at[d_place, :], inside.at[0]),
        pltpu.make_async_copy(q_ref, rows_ref.at[q_place, :], inside.at[1]),
        pltpu.make_async_copy(p_ref, marks.at[place_of_row(0, 0)], inside.at[2]),
    ]
    for copy in taken:
        copy.start()
    meet([*neighbours("y"), *neighbours("x"), sibling])
    for copy in taken:
        copy.wait()
    lse[...] = jnp.zeros_like(lse)
    peaks[...] = jnp.zeros_like(peaks)
    gather(send, rows_ref, docs_ref, own)
    mark = marks.at[place_of_row(0, 0)]
    marked = [send(mark, mark, device) for _, _, device in row_peers()]

    turn = width // 2
    tall = count // 2

    def turn_cols(part, nested=0):
        start = nested * width + part * turn
        return slice(start, start + turn)

    def score(part):
        cols_q = turn_cols(part)
        best[...] = jnp.full(best.shape, -jnp.inf, jnp.float32)

        def keep(nested, at, value):
            logits[nested, at, cols_q] = value
            top = jnp.max(value.reshape(tall // 8, 8, turn), axis=0)
            best[nested] = jnp.maximum(best[nested], top)

        def score_block(block, carry):
            at = pl.ds(pl.multiple_of(block * tall, tall), tall)
            lane = lax.broadcasted_iota(jnp.int32, (tall, narrow), 1)
            head = docs_ref[at, :narrow]
            for nested in range(few):
                cut = jnp.where(lane < uppers[nested], head, jnp.zeros_like(head))
                keep(nested, at, contract(cut, rows_ref[cols_q, :narrow], 1, 1))
            for nested in range(few, WIDTHS):
                cols = slice(lowers[nested], uppers[nested])
                more = contract(docs_ref[at, cols], rows_ref[cols_q, cols], 1, 1)
                keep(nested, at, logits[nested - 1, at, cols_q] + more)
            return carry

        lax.fori_loop(0, count // tall, score_block, 0)

    def soften(part):
        cols_q = turn_cols(part)
        tops = [jnp.max(best[nested], axis=0, keepdims=True) for nested in range(WIDTHS)]
        mass[...] = jnp.zeros_like(mass)
        size = 128

        def mass_block(block, carry):
            at = pl.ds(pl.multiple_of(block * size, size), size)
            for nested in range(WIDTHS):
                piece = logits[nested, at, cols_q] - tops[nested]
                piece = jnp.exp2(piece * (scales[nested] * LOG2_E))
                logits[nested, at, cols_q] = piece
                mass[nested] += jnp.sum(piece.reshape(size // 8, 8, turn), axis=0)
            return carry

        lax.fori_loop(0, count // size, mass_block, 0)
        for nested in range(WIDTHS):
            top = tops[nested] * scales[nested]
            value = top + jnp.log(jnp.sum(mass[nested], axis=0, keepdims=True))
            if nested < 8:
                peaks[part, nested : nested + 1, :turn] = top
                lse[part, nested : nested + 1, :turn] = value
            else:
                for line in range(turn // 128):
                    cols = slice(line * 128, (line + 1) * 128)
                    peaks[part, line : line + 1, turn:] = top[:, cols]
                    lse[part, line : line + 1, turn:] = value[:, cols]

    def share(part):
        return [
            send(lse.at[part], parts.at[part, (chips - step) % chips * 2 + pair - 1], device)
            for step, pair, device in row_peers()
        ]

    def factors(part, copies):
        for copy in copies:
            copy.wait_recv()
        pieces = [lse[part]] + [parts[part, number] for number in range(len(copies))]
        peak = functools.reduce(jnp.maximum, pieces)
        total = peak + jnp.log(sum(jnp.exp(piece - peak) for piece in pieces))
        ratio = jnp.exp(peaks[part] - total)
        rows = [ratio[nested : nested + 1, :turn] * scales[nested] for nested in range(8)]
        tail = [ratio[line : line + 1, turn:] for line in range(turn // 128)]
        return rows + [jnp.concatenate(tail, axis=1) * scales[8]]

    def band(part, factor, partner):
        cols_q = turn_cols(part)

        def band_block(block, carry):
            at = pl.ds(pl.multiple_of(block * own, own), own)
            ids = first_id(block, own) + lax.broadcasted_iota(jnp.int32, (own, turn), 0)
            hit = ids == partner[:, cols_q]
            running = jnp.zeros((own, turn), jnp.float32)
            gone = 0.0
            for nested in reversed(range(WIDTHS)):
                running = running + logits[nested, at, cols_q] * factor[nested]
                gone += scales[nested]
                value = running - jnp.where(hit, gone, 0.0)
                bands[at, turn_cols(part, nested)] = value.astype(jnp.bfloat16)
            return carry

        lax.fori_loop(0, count // own, band_block, 0)

    edge = split_at(dim)
    early, late = slice(0, edge), slice(edge, dim)

    def bounds(nested):
        return slice(0, narrow) if nested < few else slice(lowers[nested], uppers[nested])

    def product(tall_rows, get, out_ref, at):
        lane = lax.broadcasted_iota(jnp.int32, (tall_rows, narrow), 1)
        head = None
        for nested in range(WIDTHS):
            part = get(nested, bounds(nested))
            if nested < few:
                head = part if head is None else jnp.where(lane < lowers[nested], head, part)
                part = head
            if nested >= few - 1:
                out_ref[at, bounds(nested)] = part

    across = {}

    def d_rows(step, pair, other, lo=0, size=own):
        start = place_of_doc(step, pair, other) * own + lo
        return pl.ds(pl.multiple_of(start, half), size)

    def documents_for(step):
        piece = 4 * own
        chip = lax.rem(lax.axis_index("x") + step, chips)
        at = pl.ds(pl.multiple_of(chip * piece, piece), piece)
        product(
            piece,
            lambda nested, cols: contract(
                bands[at, nested * width : (nested + 1) * width], rows_ref[:, cols], 1, 0
            ),
            pd_ref,
            at,
        )
        for pair, cols in ((1, late), (1, early), (0, early), (0, late)):
            across[step, pair, cols.start] = send(
                pd_ref.at[d_rows(step, pair, 1), cols], sib.at[step * 2 + pair, :, cols], sibling
            )

    def queries_at(chip):
        piece = 2 * own
        product(
            piece,
            lambda nested, cols: contract(
                bands[:, pl.ds(pl.multiple_of(nested * width + chip * piece, piece), piece)],
                docs_ref[:, cols],
                0,
                0,
            ),
            pq_ref,
            pl.ds(pl.multiple_of(chip * piece, piece), piece),
        )

    def q_part(step, pair, lo, size, cols):
        start = place_of_row(step, pair) * own + lo
        return pq_ref[pl.ds(pl.multiple_of(start, half), size), cols]

    def d_part(step, pair, lo, size, cols):
        arrive(across[step, pair, cols.start])
        mine = pd_ref[d_rows(step, pair, 0, lo, size), cols]
        return mine + sib[step * 2 + pair, pl.ds(lo, size), cols]

    waited = []

    def arrive(copy):
        if not any(copy is seen for seen in waited):
            copy.wait_recv()
            waited.append(copy)

    lanes = ((q_part, *neighbours("y")), (d_part, *neighbours("x")))
    crossed, far, near = {}, {}, {}

    def cross(which, step):
        part, _, _, pair = lanes[which]
        cross_s[which, step] = part(step, 1, 0, own, late).astype(jnp.bfloat16)
        crossed[which, step] = send(cross_s.at[which, step], cross_r.at[which, step], pair)

    def term(which, pair, cols, step, lo, size):
        value = lanes[which][0](step, pair, lo, size, cols)
        if cols is late:
            arrive(crossed[which, step])
            value = value + cross_r[which, step, pl.ds(lo, size), :].astype(jnp.float32)
        return value

    def send_far(which, pair, cols):
        _, up, down, _ = lanes[which]
        far_s[which, pair, :, cols] = term(which, pair, cols, 2, 0, own).astype(jnp.bfloat16)
        for way, device in ((0, up), (1, down)):
            piece = pl.ds(way * half, half)
            far[which, pair, cols.start, way] = send(
                far_s.at[which, pair, piece, cols], far_r.at[which, pair, piece, cols], device
            )

    def send_near(which, pair, cols):
        _, up, down, _ = lanes[which]
        for way, device, step in ((0, up, 1), (1, down, 3)):
            lo = way * half
            more = half - lo
            near_s[which, pair, way, pl.ds(more, half), cols] = term(
                which, pair, cols, step, more, half
            ).astype(jnp.bfloat16)
            mine = term(which, pair, cols, step, lo, half)
            arrive(far[which, pair, cols.start, way])
            near_s[which, pair, way, pl.ds(lo, half), cols] = (
                mine + far_r[which, pair, pl.ds(lo, half), cols].astype(jnp.float32)
            ).astype(jnp.bfloat16)
            near[which, pair, cols.start, way] = send(
                near_s.at[which, pair, way, :, cols], near_r.at[which, pair, way, :, cols], device
            )

    def summed(which, pair, cols):
        value = term(which, pair, cols, 0, 0, own)
        for way in range(2):
            arrive(near[which, pair, cols.start, way])
            value = value + near_r[which, pair, way, :, cols].astype(jnp.float32)
        return value

    shared = []
    for part in range(2):
        score(part)
        soften(part)
        shared.append(share(part))
    for copy in marked:
        copy.wait_recv()
    partner = jnp.concatenate([marks[place] for place in range(2 * chips)], axis=1)
    band(0, factors(0, shared[0]), partner)
    queries_at(0)
    queries_at(1)
    band(1, factors(1, shared[1]), partner)
    documents_for(2)
    odd = lax.rem(lax.axis_index("y"), 2)
    queries_at(2 + odd)
    cross(0, 2)
    send_far(0, 1, early)
    send_far(0, 0, early)
    cross(0, 0)
    documents_for(1)
    cross(1, 2)
    send_far(1, 1, early)
    send_far(1, 0, early)
    queries_at(3 - odd)
    cross(1, 1)
    cross(0, 1)
    cross(0, 3)
    documents_for(3)
    send_near(0, 1, early)
    cross(1, 3)
    send_far(0, 0, late)
    send_near(1, 1, early)
    send_far(1, 0, late)
    documents_for(0)
    cross(1, 0)
    for which in (0, 1):
        send_near(which, 0, early)
    for which in (0, 1):
        send_near(which, 0, late)
    outs = (gq_ref, gd_ref)
    last = []
    for which in range(2):
        pair_s[which] = summed(which, 1, early).astype(jnp.bfloat16)
        last.append(send(pair_s.at[which], pair_r.at[which], lanes[which][3]))
    for which in range(2):
        outs[which][:, early] = summed(which, 0, early)
    for which in range(2):
        outs[which][:, late] = summed(which, 0, late)
    for which in range(2):
        last[which].wait_recv()
        outs[which][:, early] = outs[which][:, early] + pair_r[which].astype(jnp.float32)
    send.finish()


def on_device(queries, documents, partner):
    own, dim = queries.shape
    width, count = 8 * own, 16 * own
    piece = pltpu.VMEM((own, dim), jnp.float32)
    wire = jnp.bfloat16
    edge = split_at(dim)
    copies = 120
    return pl.pallas_call(
        step_kernel,
        out_shape=(piece, piece),
        in_specs=[pl.BlockSpec(memory_space=pl.ANY)] * 3,
        out_specs=(VMEM, VMEM),
        scratch_shapes=[
            pltpu.VMEM((width, dim), wire),
            pltpu.VMEM((count, dim), wire),
            pltpu.VMEM((WIDTHS, count, width), jnp.float32),
            pltpu.VMEM((count, WIDTHS * width), wire),
            pltpu.VMEM((WIDTHS, 8, width // 2), jnp.float32),
            pltpu.VMEM((WIDTHS, 8, width // 2), jnp.float32),
            pltpu.VMEM((2, 8, width // 2 + 128), jnp.float32),
            pltpu.VMEM((2, 8, width // 2 + 128), jnp.float32),
            pltpu.VMEM((2, 7, 8, width // 2 + 128), jnp.float32),
            pltpu.VMEM((8, 1, own), jnp.int32),
            pltpu.VMEM((width, dim), jnp.float32),
            pltpu.VMEM((count, dim), jnp.float32),
            pltpu.VMEM((8, own, dim), jnp.float32),
            pltpu.VMEM((2, 2, own, dim), wire),
            pltpu.VMEM((2, 2, 2, own, dim), wire),
            pltpu.VMEM((2, 2, own, dim), wire),
            pltpu.VMEM((2, 2, 2, own, dim), wire),
            pltpu.VMEM((2, own, edge), wire),
            pltpu.VMEM((2, own, edge), wire),
            pltpu.VMEM((2, 4, own, dim - edge), wire),
            pltpu.VMEM((2, 4, own, dim - edge), wire),
            pltpu.SemaphoreType.DMA((3,)),
            pltpu.SemaphoreType.DMA((copies,)),
            pltpu.SemaphoreType.DMA((copies,)),
        ],
        compiler_params=pltpu.CompilerParams(
            collective_id=0, has_side_effects=True, vmem_limit_bytes=60 * 2**20
        ),
        name="step",
    )(queries, documents, partner[None, :])


def solution(mesh):
    finer = Mesh(mesh.devices.reshape(4, 2, 4, 2, mesh.shape["rep"]), AXES)
    placed = (P(AXES, None), P(AXES, None), P(AXES))
    return jax.shard_map(
        on_device,
        mesh=finer,
        in_specs=placed,
        out_specs=(P(AXES, None), P(AXES, None)),
        check_vma=False,
    )
```
